32 devices in a mesh: slab: 8 (over y, x, core), trace: 4 (over z).
Axes of the slice: x: 2, y: 2, z: 4, core: 2. Of those that a mesh axis runs over, the one named last changes fastest.
Arguments:
- transmission: bfloat16 [8, 2048, 2048], P('slab', None, 'trace'), may hold values from -0.125 to 0.125
- reflection: bfloat16 [8, 2048, 2048], P('slab', None, 'trace'), may hold values from -0.0625 to 0.0625
- response: bfloat16 [8, 2048, 2048], P('slab', None, 'trace'), may hold values from -0.125 to 0.125
- sources: bfloat16 [8, 8, 32, 2048], P('slab', None, None, 'trace'), may hold values from -6 to 6
- placement: int32 [8, 32], replicated, may hold values from 0 to 7
Outputs:
- field_trace: bfloat16 [8, 8, 32, 2048], P('slab', None, None, 'trace')
The draws below stay inside these ranges and needn't reach their ends.
All inputs are finite; a program needn't handle non-finite values.
Results may differ from the reference program's by a relative error of at most 0.018.
Values may be sent and summed in bfloat16 or wider, within the bound.
No kernel may reach another device: no remote copies, remote signals or barrier semaphores. Data moves between devices by JAX's collectives and lax.ppermute only.
A program may use at most 64 MiB of HBM per device.

```python
import jax
import jax.numpy as jnp
from jax import lax

TW = 2048
BATCH = 32
TICKS = 8
SLABS = 8


def touch_ends(result, rng, least, top_value):
    place = [jax.random.randint(jax.random.fold_in(rng, axis), (), 0, length) for axis, length in enumerate(result.shape)]
    widest = result.shape.index(max(result.shape))
    next_to = place[:widest] + [(place[widest] + 1) % result.shape[widest]] + place[widest + 1:]
    return result.at[tuple(place)].set(least).at[tuple(next_to)].set(top_value)


def shard_levels(key, shape, pieces, smallest, high):
    def one(axis_at, blocks):
        draws = jax.random.uniform(jax.random.fold_in(jax.random.fold_in(key, 6), axis_at), (blocks,), jnp.float32, smallest / len(pieces), high / len(pieces))
        return jnp.repeat(jnp.exp(draws), shape[axis_at] // blocks).reshape((-1,) + (1,) * (len(shape) - axis_at - 1))

    gain = one(*pieces[0])
    for cut in pieces[1:]:
        gain = gain * one(*cut)
    return gain


def scatter_about(own_key, shape, spread, limit, split=(), kind=jnp.bfloat16):
    array = spread * jax.random.normal(own_key, shape, jnp.float32)
    if split:
        array = array * shard_levels(own_key, shape, split, -0.22, 0.18)
    return jnp.clip(array, -limit, limit).astype(kind)


def setup_inputs(seed: int = 0) -> dict:
    key_of = jax.random.split(jax.random.key(seed), 6)
    transmission = scatter_about(key_of[0], (SLABS, TW, TW), (TW + TW // 9) ** -0.5, 0.125, ((0, 8), (2, 4)))
    reflection = scatter_about(key_of[1], (SLABS, TW, TW), (4 * TW) ** -0.5, 0.0625, ((0, 8), (2, 4)))
    response = scatter_about(key_of[2], (SLABS, TW, TW), TW ** -0.5, 0.125, ((0, 8), (2, 4)))
    sources = scatter_about(key_of[3], (SLABS, TICKS, BATCH, TW), 1.0, 6.0, ((0, 8), (3, 4)))
    placement = touch_ends(jax.random.randint(key_of[4], (TICKS, BATCH), 0, SLABS), jax.random.fold_in(key_of[4], 1), 0, SLABS - 1).astype(jnp.int32)
    return {"transmission": transmission, "reflection": reflection, "response": response, "sources": sources, "placement": placement}


def reference(transmission, reflection, response, sources, placement):
    slab_ids = jnp.arange(SLABS, dtype=jnp.int32)
    distance = jnp.abs(slab_ids[:, None, None] - placement[None, :, :]).astype(jnp.float32)
    weighting = 1.0 / (1.0 + distance)
    weighted = (sources.astype(jnp.float32) * weighting[..., None]).astype(jnp.bfloat16)
    flat = weighted.reshape(SLABS, TICKS * BATCH, TW)

    def respond(pair):
        return jnp.dot(pair[0], pair[1], preferred_element_type=jnp.float32)

    driven = lax.map(respond, (flat, response))

    def carry_along(incoming, pair):
        matrix, driven_here = pair
        fresh = (jnp.dot(incoming, matrix, preferred_element_type=jnp.float32) + driven_here).astype(jnp.bfloat16)
        return fresh, fresh

    initial = jnp.zeros((TICKS * BATCH, TW), jnp.bfloat16)
    ignored, down = lax.scan(carry_along, initial, (transmission, driven))
    ignored_up, up = lax.scan(carry_along, initial, (transmission, driven), reverse=True)
    contrast = (down.astype(jnp.float32) - up.astype(jnp.float32)).astype(jnp.bfloat16)

    def combine(quad):
        reflected = jnp.dot(quad[0], quad[3], preferred_element_type=jnp.float32)
        return (quad[1].astype(jnp.float32) + quad[2].astype(jnp.float32) + reflected).astype(jnp.bfloat16)

    field_trace = lax.map(combine, (contrast, down, up, reflection))
    return field_trace.reshape(SLABS, TICKS, BATCH, TW)
```

```python
import jax
import jax.numpy as jnp
from jax import lax
from jax.sharding import PartitionSpec as P

AXES = ("slab", "trace")
CHUNKS = 2


class Places:
    def __init__(self, slab_count, trace_count):
        self.columns = slab_count // 2
        self.width = trace_count
        self.holders = (trace_count // 2 - 1, trace_count // 2)
        self.extra = trace_count // 2 - 1

    def at(self, column, core, z):
        return (2 * column + core) * self.width + z

    def everyone(self):
        return [(c, k, z) for c in range(self.columns) for k in (0, 1) for z in range(self.width)]

    def working(self, stage):
        return ((stage, 0), (self.columns - 1 - stage, 1))

    def partner_map(self):
        return {self.at(c, k, z): self.at(c, 1 - k, z) for c, k, z in self.everyone()}

    def across_cores(self):
        return list(self.partner_map().items())

    def swap(self, stage):
        moves = self.partner_map()
        (ca, ka), (cb, kb) = self.working(stage)
        low, high = self.holders
        for z, other in ((low, high), (high, low)):
            for c, k in ((ca, ka), (cb, kb)):
                moves[self.at(c, k, z)] = self.at(c, k, other)
            if ca != cb:
                moves[self.at(ca, 1 - ka, z)] = self.at(cb, 1 - kb, z)
                moves[self.at(cb, 1 - kb, z)] = self.at(ca, 1 - ka, z)
        return list(moves.items())

    def swap_all(self):
        moves = self.partner_map()
        low, high = self.holders
        for c in range(self.columns):
            for k in (0, 1):
                moves[self.at(c, k, low)] = self.at(c, k, high)
                moves[self.at(c, k, high)] = self.at(c, k, low)
        return list(moves.items())

    def hop(self, stage, crossed):
        moves = self.partner_map()
        low, high = self.holders
        for z, other in ((low, high), (high, low)):
            for (before, k), (after, _) in zip(self.working(stage - 1), self.working(stage)):
                moves[self.at(before, k, z)] = self.at(after, k, other if crossed else z)
                if 2 * stage != self.columns:
                    moves[self.at(after, 1 - k, z)] = self.at(before, 1 - k, z)
        return list(moves.items())

    def ends(self, hop):
        low, high = self.holders
        return ((low - hop, low), (high + hop, high))

    def exchange_end(self, hop):
        moves = []
        for c in range(self.columns):
            for k in (0, 1):
                for end, holder in self.ends(hop):
                    moves += [(self.at(c, k, end), self.at(c, k, holder)), (self.at(c, k, holder), self.at(c, k, end))]
        return moves

    def inward(self, hop):
        return [
            (self.at(c, k, end), self.at(c, k, holder))
            for c in range(self.columns) for k in (0, 1) for end, holder in self.ends(hop)
        ]

    def first_sender(self, column):
        if column < self.columns // 2:
            return 1 if column == 0 else 0
        return 1 - self.first_sender(self.columns - 1 - column)

    def inward_crossed(self, hop, early):
        moves = []
        for c in range(self.columns):
            k = self.first_sender(c) if early else 1 - self.first_sender(c)
            for end, holder in self.ends(hop):
                moves.append((self.at(c, k, end), self.at(c, 1 - k, holder)))
        return moves


def move(values, pairs):
    return lax.ppermute(values, AXES, pairs)


def joined(pieces):
    return pieces if len(pieces) < 2 else [jnp.concatenate(pieces, 1)]


def dot32(rows, matrix):
    return jnp.dot(rows, matrix, preferred_element_type=jnp.float32)


def by_half(matrix, places, lower):
    depth = matrix.shape[0] // places.width
    low, high = places.holders
    down = [matrix[i * depth:(i + 1) * depth] for i in range(low, -1, -1)]
    up = [matrix[i * depth:(i + 1) * depth] for i in range(high, places.width)]
    return jnp.where(lower, jnp.concatenate(down + up, 0), jnp.concatenate(up + down, 0))


def times(own_rows, other_rows, pieces):
    half = own_rows.shape[1]
    return jnp.concatenate(
        [dot32(own_rows, piece[:half]) + dot32(other_rows, piece[half:]) for piece in pieces], 1
    )


def shards(transmission, reflection, response, sources, placement):
    own_sources = sources[0]
    tick_count, batch_count, trace_width = own_sources.shape
    total_rows = tick_count * batch_count
    slab_index = lax.axis_index("slab")
    z = lax.axis_index("trace")
    trace_count = lax.axis_size("trace")
    places = Places(lax.axis_size("slab"), trace_count)
    core = slab_index % 2
    column = slab_index // 2
    my_stage = jnp.where(core == 0, column, places.columns - 1 - column)
    lower = z <= places.holders[0]
    hops = range(1, places.extra + 1)

    distance = jnp.abs(slab_index - placement).astype(jnp.float32)
    weighting = 1.0 / (1.0 + distance)
    weighted = (own_sources.astype(jnp.float32) * weighting[:, :, None]).astype(jnp.bfloat16)
    flat = weighted.reshape(total_rows, trace_width)

    gathered = [flat] + [
        lax.ppermute(flat, "trace", [(i, (i + k) % trace_count) for i in range(trace_count)])
        for k in range(1, trace_count)
    ]
    respond = response[0]
    driven = jnp.zeros((total_rows, trace_width), jnp.float32)
    for k, rows in enumerate(gathered):
        block = lax.rem(z - k + trace_count, trace_count)
        driven = driven + dot32(rows, lax.dynamic_slice_in_dim(respond, block * trace_width, trace_width, 0))

    transfer = by_half(transmission[0], places, lower)
    reflect = by_half(reflection[0], places, lower)
    second_own = move(transfer, places.across_cores())
    second_early = joined([move(transfer, places.inward_crossed(hop, True)) for hop in hops])
    first_early = [move(piece, places.across_cores()) for piece in second_early]
    second_late = joined([move(transfer, places.inward_crossed(hop, False)) for hop in hops])
    first_late = [move(piece, places.across_cores()) for piece in second_late]
    reflect_rest = joined([move(reflect, places.inward(hop)) for hop in hops])

    driven_sent = driven.astype(jnp.bfloat16)
    first_driven = jnp.concatenate(
        [driven_sent] + [move(driven_sent, places.exchange_end(hop)) for hop in hops], 1
    )
    second_driven = move(first_driven, places.across_cores())

    step = total_rows // CHUNKS

    def split(values):
        return [values[i * step:(i + 1) * step] for i in range(CHUNKS)]

    firsts, seconds = [None] * CHUNKS, [None] * CHUNKS

    def kept(results, stage, fresh):
        return [new if old is None else jnp.where(my_stage == stage, new, old) for old, new in zip(results, fresh)]

    first_parts, second_parts = split(first_driven), split(second_driven)
    traces = first_parts
    for stage in range(places.columns):
        early = places.first_sender(stage) == 0
        first_pieces = [transfer] + (first_early if early else first_late)
        second_pieces = [second_own] + (second_late if early else second_early)
        if stage:
            arrived = [
                (move(part, places.hop(stage, True)), move(part, places.hop(stage, False))) for part in traces
            ]
            traces = [
                (times(straight, crossed, first_pieces) + extra).astype(jnp.bfloat16)
                for (crossed, straight), extra in zip(arrived, first_parts)
            ]
        firsts = kept(firsts, stage, traces)
        others = [move(part, places.swap(stage)) for part in traces]
        traces = [
            (times(part, other, second_pieces) + extra).astype(jnp.bfloat16)
            for part, other, extra in zip(traces, others, second_parts)
        ]
        seconds = kept(seconds, stage, traces)

    outs = []
    for part in range(CHUNKS):
        mine = firsts[part].astype(jnp.float32)
        opposite = move(seconds[part], places.across_cores()).astype(jnp.float32)
        contrast = jnp.where(core == 0, mine - opposite, opposite - mine).astype(jnp.bfloat16)
        other = move(contrast, places.swap_all())
        combined = (times(contrast, other, [reflect] + reflect_rest) + mine + opposite).astype(jnp.bfloat16)
        own = combined[:, :trace_width]
        for hop in hops:
            piece = move(combined[:, hop * trace_width:(hop + 1) * trace_width], places.exchange_end(hop))
            own = jnp.where((z == places.ends(hop)[0][0]) | (z == places.ends(hop)[1][0]), piece, own)
        outs.append(own)
    return jnp.concatenate(outs, 0).reshape(1, tick_count, batch_count, trace_width)


def solution(mesh):
    placed = (
        P("slab", None, "trace"),
        P("slab", None, "trace"),
        P("slab", None, "trace"),
        P("slab", None, None, "trace"),
        P(),
    )
    return jax.shard_map(
        shards,
        mesh=mesh,
        in_specs=placed,
        out_specs=P("slab", None, None, "trace"),
        check_vma=False,
    )
```

```python
import functools

import jax
import jax.numpy as jnp
from jax import lax
from jax.experimental import pallas as pl
from jax.experimental.pallas import tpu as pltpu
from jax.sharding import PartitionSpec as P

AXES = ("slab", "trace")
CHUNKS = 2


class Places:
    def __init__(self, slab_count, trace_count):
        self.columns = slab_count // 2
        self.width = trace_count
        self.holders = (trace_count // 2 - 1, trace_count // 2)
        self.extra = trace_count // 2 - 1

    def at(self, column, core, z):
        return (2 * column + core) * self.width + z

    def everyone(self):
        return [(c, k, z) for c in range(self.columns) for k in (0, 1) for z in range(self.width)]

    def working(self, stage):
        return ((stage, 0), (self.columns - 1 - stage, 1))

    def partner_map(self):
        return {self.at(c, k, z): self.at(c, 1 - k, z) for c, k, z in self.everyone()}

    def across_cores(self):
        return list(self.partner_map().items())

    def swap(self, stage):
        moves = self.partner_map()
        (ca, ka), (cb, kb) = self.working(stage)
        low, high = self.holders
        for z, other in ((low, high), (high, low)):
            for c, k in ((ca, ka), (cb, kb)):
                moves[self.at(c, k, z)] = self.at(c, k, other)
            if ca != cb:
                moves[self.at(ca, 1 - ka, z)] = self.at(cb, 1 - kb, z)
                moves[self.at(cb, 1 - kb, z)] = self.at(ca, 1 - ka, z)
        return list(moves.items())

    def swap_all(self):
        moves = self.partner_map()
        low, high = self.holders
        for c in range(self.columns):
            for k in (0, 1):
                moves[self.at(c, k, low)] = self.at(c, k, high)
                moves[self.at(c, k, high)] = self.at(c, k, low)
        return list(moves.items())

    def hop(self, stage, crossed):
        moves = self.partner_map()
        low, high = self.holders
        for z, other in ((low, high), (high, low)):
            for (before, k), (after, _) in zip(self.working(stage - 1), self.working(stage)):
                moves[self.at(before, k, z)] = self.at(after, k, other if crossed else z)
                if 2 * stage != self.columns:
                    moves[self.at(after, 1 - k, z)] = self.at(before, 1 - k, z)
        return list(moves.items())

    def ends(self, hop):
        low, high = self.holders
        return ((low - hop, low), (high + hop, high))

    def exchange_end(self, hop):
        moves = []
        for c in range(self.columns):
            for k in (0, 1):
                for end, holder in self.ends(hop):
                    moves += [(self.at(c, k, end), self.at(c, k, holder)), (self.at(c, k, holder), self.at(c, k, end))]
        return moves

    def inward(self, hop):
        return [
            (self.at(c, k, end), self.at(c, k, holder))
            for c in range(self.columns) for k in (0, 1) for end, holder in self.ends(hop)
        ]

    def first_sender(self, column):
        if column < self.columns // 2:
            return 1 if column == 0 else 0
        return 1 - self.first_sender(self.columns - 1 - column)

    def inward_crossed(self, hop, early):
        moves = []
        for c in range(self.columns):
            k = self.first_sender(c) if early else 1 - self.first_sender(c)
            for end, holder in self.ends(hop):
                moves.append((self.at(c, k, end), self.at(c, 1 - k, holder)))
        return moves


def move(values, pairs):
    return lax.ppermute(values, AXES, pairs)


def joined(pieces):
    return pieces if len(pieces) < 2 else [jnp.concatenate(pieces, 1)]


def dot32(rows, matrix):
    return jnp.dot(rows, matrix, preferred_element_type=jnp.float32)


def apply_kernel(width, own_ref, other_ref, near_ref, far_ref, add_ref, out_ref, near_tiles, far_tiles, sems):
    depth = near_ref.shape[0] // width
    half = width // 2
    lower = lax.axis_index("trace") < half
    down = [half - 1 - i for i in range(half)]
    up = [half + i for i in range(half)]
    blocks = [jnp.where(lower, x, y) for x, y in zip(down + up, up + down)]
    copies = []
    for t, block in enumerate(blocks):
        rows = pl.ds(pl.multiple_of(block * depth, depth), depth)
        pair = (
            pltpu.make_async_copy(near_ref.at[rows, :], near_tiles.at[t], sems.at[0, t]),
            pltpu.make_async_copy(far_ref.at[rows, :], far_tiles.at[t], sems.at[1, t]),
        )
        for copy in pair:
            copy.start()
        copies.append(pair)
    near = far = 0.0
    for t, pair in enumerate(copies):
        source = own_ref if t < half else other_ref
        rows = source[:, (t % half) * depth:(t % half + 1) * depth]
        for copy in pair:
            copy.wait()
        near += jnp.dot(rows, near_tiles[t], preferred_element_type=jnp.float32)
        far += jnp.dot(rows, far_tiles[t], preferred_element_type=jnp.float32)
    cut = near_ref.shape[1]
    out_ref[:, :cut] = (near + add_ref[:, :cut]).astype(out_ref.dtype)
    out_ref[:, cut:] = (far + add_ref[:, cut:]).astype(out_ref.dtype)


def applied(own, other, pieces, addend):
    near, far = pieces
    width = lax.axis_size("trace")
    rows, columns = addend.shape
    depth = near.shape[0] // width
    vmem = pl.BlockSpec(memory_space=pltpu.VMEM)
    hbm = pl.BlockSpec(memory_space=pltpu.HBM)
    return pl.pallas_call(
        functools.partial(apply_kernel, width),
        out_shape=jax.ShapeDtypeStruct((rows, columns), jnp.bfloat16),
        in_specs=[vmem, vmem, hbm, hbm, vmem],
        out_specs=vmem,
        scratch_shapes=[
            pltpu.VMEM((width, depth, near.shape[1]), near.dtype),
            pltpu.VMEM((width, depth, far.shape[1]), far.dtype),
            pltpu.SemaphoreType.DMA((2, width)),
        ],
        compiler_params=pltpu.CompilerParams(vmem_limit_bytes=16 * 1024 * 1024),
        cost_estimate=pl.CostEstimate(
            flops=2 * rows * columns * near.shape[0], bytes_accessed=2 * columns * near.shape[0], transcendentals=0
        ),
    )(own, other, near, far, addend)


def shards(transmission, reflection, response, sources, placement):
    own_sources = sources[0]
    tick_count, batch_count, trace_width = own_sources.shape
    total_rows = tick_count * batch_count
    slab_index = lax.axis_index("slab")
    z = lax.axis_index("trace")
    trace_count = lax.axis_size("trace")
    places = Places(lax.axis_size("slab"), trace_count)
    core = slab_index % 2
    column = slab_index // 2
    my_stage = jnp.where(core == 0, column, places.columns - 1 - column)
    hops = range(1, places.extra + 1)

    distance = jnp.abs(slab_index - placement).astype(jnp.float32)
    weighting = 1.0 / (1.0 + distance)
    weighted = (own_sources.astype(jnp.float32) * weighting[:, :, None]).astype(jnp.bfloat16)
    flat = weighted.reshape(total_rows, trace_width)

    gathered = [flat] + [
        lax.ppermute(flat, "trace", [(i, (i + k) % trace_count) for i in range(trace_count)])
        for k in range(1, trace_count)
    ]
    respond = response[0]
    driven = jnp.zeros((total_rows, trace_width), jnp.float32)
    for k, rows in enumerate(gathered):
        block = lax.rem(z - k + trace_count, trace_count)
        driven = driven + dot32(rows, lax.dynamic_slice_in_dim(respond, block * trace_width, trace_width, 0))

    transfer = transmission[0]
    reflect = reflection[0]
    second_own = move(transfer, places.across_cores())
    second_early = joined([move(transfer, places.inward_crossed(hop, True)) for hop in hops])
    first_early = [move(piece, places.across_cores()) for piece in second_early]
    second_late = joined([move(transfer, places.inward_crossed(hop, False)) for hop in hops])
    first_late = [move(piece, places.across_cores()) for piece in second_late]
    reflect_rest = joined([move(reflect, places.inward(hop)) for hop in hops])

    driven_sent = driven.astype(jnp.bfloat16)
    first_driven = jnp.concatenate(
        [driven_sent] + [move(driven_sent, places.exchange_end(hop)) for hop in hops], 1
    )
    second_driven = move(first_driven, places.across_cores())

    step = total_rows // CHUNKS

    def split(values):
        return [values[i * step:(i + 1) * step] for i in range(CHUNKS)]

    firsts, seconds = [], []

    def chosen(stages, part):
        result = stages[0][part]
        for stage in range(1, places.columns):
            result = jnp.where(my_stage == stage, stages[stage][part], result)
        return result

    first_parts, second_parts = split(first_driven), split(second_driven)
    traces = first_parts
    for stage in range(places.columns):
        early = places.first_sender(stage) == 0
        first_pieces = [transfer] + (first_early if early else first_late)
        second_pieces = [second_own] + (second_late if early else second_early)
        if stage:
            arrived = [
                (move(part, places.hop(stage, True)), move(part, places.hop(stage, False))) for part in traces
            ]
            traces = [
                applied(straight, crossed, first_pieces, extra)
                for (crossed, straight), extra in zip(arrived, first_parts)
            ]
        firsts.append(traces)
        others = [move(part, places.swap(stage)) for part in traces]
        traces = [
            applied(part, other, second_pieces, extra)
            for part, other, extra in zip(traces, others, second_parts)
        ]
        seconds.append(traces)

    outs = []
    for part in range(CHUNKS):
        mine = chosen(firsts, part).astype(jnp.float32)
        opposite = move(chosen(seconds, part), places.across_cores()).astype(jnp.float32)
        contrast = jnp.where(core == 0, mine - opposite, opposite - mine).astype(jnp.bfloat16)
        other = move(contrast, places.swap_all())
        combined = applied(contrast, other, [reflect] + reflect_rest, mine + opposite)
        own = combined[:, :trace_width]
        for hop in hops:
            piece = move(combined[:, hop * trace_width:(hop + 1) * trace_width], places.exchange_end(hop))
            own = jnp.where((z == places.ends(hop)[0][0]) | (z == places.ends(hop)[1][0]), piece, own)
        outs.append(own)
    return jnp.concatenate(outs, 0).reshape(1, tick_count, batch_count, trace_width)


def solution(mesh):
    placed = (
        P("slab", None, "trace"),
        P("slab", None, "trace"),
        P("slab", None, "trace"),
        P("slab", None, None, "trace"),
        P(),
    )
    return jax.shard_map(
        shards,
        mesh=mesh,
        in_specs=placed,
        out_specs=P("slab", None, None, "trace"),
        check_vma=False,
    )
```

```python
import functools

import jax
import jax.numpy as jnp
from jax import lax
from jax.experimental import pallas as pl
from jax.experimental.pallas import tpu as pltpu
from jax.sharding import PartitionSpec as P


AXES = ("slab", "trace")
CHUNKS = 2


class Places:
    def __init__(self, slab_count, trace_count):
        self.columns = slab_count // 2
        self.width = trace_count
        self.holders = (trace_count // 2 - 1, trace_count // 2)
        self.extra = trace_count // 2 - 1

    def at(self, column, core, z):
        return (2 * column + core) * self.width + z

    def everyone(self):
        return [(c, k, z) for c in range(self.columns) for k in (0, 1) for z in range(self.width)]

    def working(self, stage):
        return ((stage, 0), (self.columns - 1 - stage, 1))

    def partner_map(self):
        return {self.at(c, k, z): self.at(c, 1 - k, z) for c, k, z in self.everyone()}

    def across_cores(self):
        return list(self.partner_map().items())

    def swap(self, stage):
        moves = self.partner_map()
        (ca, ka), (cb, kb) = self.working(stage)
        low, high = self.holders
        for z, other in ((low, high), (high, low)):
            for c, k in ((ca, ka), (cb, kb)):
                moves[self.at(c, k, z)] = self.at(c, k, other)
            if ca != cb:
                moves[self.at(ca, 1 - ka, z)] = self.at(cb, 1 - kb, z)
                moves[self.at(cb, 1 - kb, z)] = self.at(ca, 1 - ka, z)
        return list(moves.items())

    def swap_all(self):
        moves = self.partner_map()
        low, high = self.holders
        for c in range(self.columns):
            for k in (0, 1):
                moves[self.at(c, k, low)] = self.at(c, k, high)
                moves[self.at(c, k, high)] = self.at(c, k, low)
        return list(moves.items())

    def hop(self, stage, crossed):
        moves = self.partner_map()
        low, high = self.holders
        for z, other in ((low, high), (high, low)):
            for (before, k), (after, _) in zip(self.working(stage - 1), self.working(stage)):
                moves[self.at(before, k, z)] = self.at(after, k, other if crossed else z)
                if 2 * stage != self.columns:
                    moves[self.at(after, 1 - k, z)] = self.at(before, 1 - k, z)
        return list(moves.items())

    def ends(self, hop):
        low, high = self.holders
        return ((low - hop, low), (high + hop, high))

    def exchange_end(self, hop):
        moves = []
        for c in range(self.columns):
            for k in (0, 1):
                for end, holder in self.ends(hop):
                    moves += [(self.at(c, k, end), self.at(c, k, holder)), (self.at(c, k, holder), self.at(c, k, end))]
        return moves

    def inward(self, hop):
        return [
            (self.at(c, k, end), self.at(c, k, holder))
            for c in range(self.columns) for k in (0, 1) for end, holder in self.ends(hop)
        ]

    def first_sender(self, column):
        if column < self.columns // 2:
            return 1 if column == 0 else 0
        return 1 - self.first_sender(self.columns - 1 - column)

    def inward_crossed(self, hop, early):
        moves = []
        for c in range(self.columns):
            k = self.first_sender(c) if early else 1 - self.first_sender(c)
            for end, holder in self.ends(hop):
                moves.append((self.at(c, k, end), self.at(c, 1 - k, holder)))
        return moves


def move(values, pairs):
    return lax.ppermute(values, AXES, pairs)


def after(values, earlier):
    return lax.optimization_barrier((values, earlier))[0]


def joined(pieces):
    return pieces if len(pieces) < 2 else [jnp.concatenate(pieces, 1)]


def dot32(rows, matrix):
    return jnp.dot(rows, matrix, preferred_element_type=jnp.float32)


def apply_kernel(width, own_ref, other_ref, near_ref, far_ref, add_ref, out_ref, near_tiles, far_tiles, sems):
    depth = near_ref.shape[0] // width
    half = width // 2
    lower = lax.axis_index("trace") < half
    down = [half - 1 - i for i in range(half)]
    up = [half + i for i in range(half)]
    blocks = [jnp.where(lower, x, y) for x, y in zip(down + up, up + down)]
    copies = []
    for t, block in enumerate(blocks):
        rows = pl.ds(pl.multiple_of(block * depth, depth), depth)
        pair = (
            pltpu.make_async_copy(near_ref.at[rows, :], near_tiles.at[t], sems.at[0, t]),
            pltpu.make_async_copy(far_ref.at[rows, :], far_tiles.at[t], sems.at[1, t]),
        )
        for copy in pair:
            copy.start()
        copies.append(pair)
    near = far = 0.0
    for t, pair in enumerate(copies):
        source = own_ref if t < half else other_ref
        rows = source[:, (t % half) * depth:(t % half + 1) * depth]
        for copy in pair:
            copy.wait()
        near += jnp.dot(rows, near_tiles[t], preferred_element_type=jnp.float32)
        far += jnp.dot(rows, far_tiles[t], preferred_element_type=jnp.float32)
    cut = near_ref.shape[1]
    out_ref[:, :cut] = (near + add_ref[:, :cut]).astype(out_ref.dtype)
    out_ref[:, cut:] = (far + add_ref[:, cut:]).astype(out_ref.dtype)


def applied(own, other, pieces, addend):
    near, far = pieces
    width = lax.axis_size("trace")
    rows, columns = addend.shape
    depth = near.shape[0] // width
    vmem = pl.BlockSpec(memory_space=pltpu.VMEM)
    hbm = pl.BlockSpec(memory_space=pltpu.HBM)
    return pl.pallas_call(
        functools.partial(apply_kernel, width),
        out_shape=jax.ShapeDtypeStruct((rows, columns), jnp.bfloat16),
        in_specs=[vmem, vmem, hbm, hbm, vmem],
        out_specs=vmem,
        scratch_shapes=[
            pltpu.VMEM((width, depth, near.shape[1]), near.dtype),
            pltpu.VMEM((width, depth, far.shape[1]), far.dtype),
            pltpu.SemaphoreType.DMA((2, width)),
        ],
        compiler_params=pltpu.CompilerParams(vmem_limit_bytes=16 * 1024 * 1024),
        cost_estimate=pl.CostEstimate(
            flops=2 * rows * columns * near.shape[0], bytes_accessed=2 * columns * near.shape[0], transcendentals=0
        ),
    )(own, other, near, far, addend)


def in_turn(rows, pieces, addends, last):
    results = []
    for (own, other), addend in zip(rows, addends):
        last = applied(after(own, last), other, pieces, addend)
        results.append(last)
    return results


def shards(transmission, reflection, response, sources, placement):
    own_sources = sources[0]
    tick_count, batch_count, trace_width = own_sources.shape
    total_rows = tick_count * batch_count
    slab_index = lax.axis_index("slab")
    z = lax.axis_index("trace")
    trace_count = lax.axis_size("trace")
    places = Places(lax.axis_size("slab"), trace_count)
    core = slab_index % 2
    column = slab_index // 2
    my_stage = jnp.where(core == 0, column, places.columns - 1 - column)
    hops = range(1, places.extra + 1)

    distance = jnp.abs(slab_index - placement).astype(jnp.float32)
    weighting = 1.0 / (1.0 + distance)
    weighted = (own_sources.astype(jnp.float32) * weighting[:, :, None]).astype(jnp.bfloat16)
    flat = weighted.reshape(total_rows, trace_width)

    gathered = [flat]
    for k in range(1, trace_count):
        gathered.append(lax.ppermute(flat, "trace", [(i, (i + k) % trace_count) for i in range(trace_count)]))
    respond = response[0]
    driven = jnp.zeros((total_rows, trace_width), jnp.float32)
    for k, rows in enumerate(gathered):
        block = lax.rem(z - k + trace_count, trace_count)
        driven = driven + dot32(rows, lax.dynamic_slice_in_dim(respond, block * trace_width, trace_width, 0))

    transfer = transmission[0]
    reflect = reflection[0]
    second_own = move(transfer, places.across_cores())
    second_early = joined([move(transfer, places.inward_crossed(hop, True)) for hop in hops])

    driven_sent = driven.astype(jnp.bfloat16)
    first_driven = jnp.concatenate(
        [driven_sent] + [move(driven_sent, places.exchange_end(hop)) for hop in hops], 1
    )
    late_source = after(transfer, first_driven)
    second_late = joined([move(late_source, places.inward_crossed(hop, False)) for hop in hops])

    step = total_rows // CHUNKS

    def split(values):
        return [values[i * step:(i + 1) * step] for i in range(CHUNKS)]

    firsts, seconds = [], []

    def chosen(stages, part):
        result = stages[0][part]
        for stage in range(1, places.columns):
            result = jnp.where(my_stage == stage, stages[stage][part], result)
        return result

    first_parts = split(first_driven)
    second_parts = split(move(first_driven, places.across_cores()))
    traces = first_parts
    for stage in range(places.columns):
        early = places.first_sender(stage) == 0
        second_pieces = [second_own] + (second_late if early else second_early)
        if stage:
            first_pieces = [transfer] + (first_early if early else first_late)
            arrived = []
            for part in traces:
                crossed = move(part, places.hop(stage, True))
                arrived.append((move(part, places.hop(stage, False)), crossed))
            traces = in_turn(arrived, first_pieces, first_parts, traces[-1])
        firsts.append(traces)
        others = []
        for part in traces:
            others.append(move(part, places.swap(stage)))
        traces = in_turn(list(zip(traces, others)), second_pieces, second_parts, traces[-1])
        seconds.append(traces)
        if stage == 0:
            first_early = [move(after(piece, traces[-1]), places.across_cores()) for piece in second_early]
        if stage == min(1, places.columns - 1):
            first_late = [move(after(piece, traces[-1]), places.across_cores()) for piece in second_late]
            reflect_source = after(reflect, traces[-1])
            reflect_rest = joined([move(reflect_source, places.inward(hop)) for hop in hops])

    outs = []
    for part in range(CHUNKS):
        mine = chosen(firsts, part).astype(jnp.float32)
        opposite = move(chosen(seconds, part), places.across_cores()).astype(jnp.float32)
        contrast = jnp.where(core == 0, mine - opposite, opposite - mine).astype(jnp.bfloat16)
        other = move(contrast, places.swap_all())
        combined = applied(contrast, other, [reflect] + reflect_rest, mine + opposite)
        own = combined[:, :trace_width]
        for hop in hops:
            piece = move(combined[:, hop * trace_width:(hop + 1) * trace_width], places.exchange_end(hop))
            own = jnp.where((z == places.ends(hop)[0][0]) | (z == places.ends(hop)[1][0]), piece, own)
        outs.append(own)
    return jnp.concatenate(outs, 0).reshape(1, tick_count, batch_count, trace_width)


def solution(mesh):
    placed = (
        P("slab", None, "trace"),
        P("slab", None, "trace"),
        P("slab", None, "trace"),
        P("slab", None, None, "trace"),
        P(),
    )

    return jax.shard_map(
        shards,
        mesh=mesh,
        in_specs=placed,
        out_specs=P("slab", None, None, "trace"),
        check_vma=False,
    )
```

```python
import functools

import jax
import jax.numpy as jnp
from jax import lax
from jax.experimental import pallas as pl
from jax.experimental.pallas import tpu as pltpu
from jax.sharding import PartitionSpec as P


AXES = ("slab", "trace")
CHUNKS = 2


class Places:
    def __init__(self, slab_count, trace_count):
        self.columns = slab_count // 2
        self.width = trace_count
        self.holders = (trace_count // 2 - 1, trace_count // 2)
        self.extra = trace_count // 2 - 1

    def at(self, column, core, z):
        return (2 * column + core) * self.width + z

    def everyone(self):
        return [(c, k, z) for c in range(self.columns) for k in (0, 1) for z in range(self.width)]

    def working(self, stage):
        return ((stage, 0), (self.columns - 1 - stage, 1))

    def partner_map(self):
        return {self.at(c, k, z): self.at(c, 1 - k, z) for c, k, z in self.everyone()}

    def across_cores(self):
        return list(self.partner_map().items())

    def swap(self, stage):
        moves = self.partner_map()
        (ca, ka), (cb, kb) = self.working(stage)
        low, high = self.holders
        for z, other in ((low, high), (high, low)):
            for c, k in ((ca, ka), (cb, kb)):
                moves[self.at(c, k, z)] = self.at(c, k, other)
            if ca != cb:
                moves[self.at(ca, 1 - ka, z)] = self.at(cb, 1 - kb, z)
                moves[self.at(cb, 1 - kb, z)] = self.at(ca, 1 - ka, z)
        return list(moves.items())

    def swap_all(self):
        moves = self.partner_map()
        low, high = self.holders
        for c in range(self.columns):
            for k in (0, 1):
                moves[self.at(c, k, low)] = self.at(c, k, high)
                moves[self.at(c, k, high)] = self.at(c, k, low)
        return list(moves.items())

    def hop(self, stage, crossed):
        moves = self.partner_map()
        low, high = self.holders
        for z, other in ((low, high), (high, low)):
            for (before, k), (after, _) in zip(self.working(stage - 1), self.working(stage)):
                moves[self.at(before, k, z)] = self.at(after, k, other if crossed else z)
                if 2 * stage != self.columns:
                    moves[self.at(after, 1 - k, z)] = self.at(before, 1 - k, z)
        return list(moves.items())

    def ends(self, hop):
        low, high = self.holders
        return ((low - hop, low), (high + hop, high))

    def exchange_end(self, hop):
        moves = []
        for c in range(self.columns):
            for k in (0, 1):
                for end, holder in self.ends(hop):
                    moves += [(self.at(c, k, end), self.at(c, k, holder)), (self.at(c, k, holder), self.at(c, k, end))]
        return moves

    def inward(self, hop):
        return [
            (self.at(c, k, end), self.at(c, k, holder))
            for c in range(self.columns) for k in (0, 1) for end, holder in self.ends(hop)
        ]

    def outward(self, hop):
        return [(holder, end) for end, holder in self.inward(hop)]

    def first_sender(self, column):
        if column < self.columns // 2:
            return 1 if column == 0 else 0
        return 1 - self.first_sender(self.columns - 1 - column)

    def inward_crossed(self, hop, early):
        moves = []
        for c in range(self.columns):
            k = self.first_sender(c) if early else 1 - self.first_sender(c)
            for end, holder in self.ends(hop):
                moves.append((self.at(c, k, end), self.at(c, 1 - k, holder)))
        return moves


def move(values, pairs):
    return lax.ppermute(values, AXES, pairs)


def after(values, earlier):
    return lax.optimization_barrier((values, earlier))[0]


def joined(pieces):
    return pieces if len(pieces) < 2 else [jnp.concatenate(pieces, 1)]


def apply_kernel(width, pieces, own_ref, other_ref, *refs):
    operators, rest = refs[:pieces], refs[pieces:]
    add_ref = rest[0] if len(rest) > pieces + 2 else None
    out_ref, tiles, sems = rest[-pieces - 2], rest[-pieces - 1:-1], rest[-1]
    depth = operators[0].shape[0] // width
    half = width // 2
    lower = lax.axis_index("trace") < half
    down = [half - 1 - i for i in range(half)]
    up = [half + i for i in range(half)]
    blocks = [jnp.where(lower, x, y) for x, y in zip(down + up, up + down)]
    copies = []
    for t, block in enumerate(blocks):
        rows = pl.ds(pl.multiple_of(block * depth, depth), depth)
        group = [
            pltpu.make_async_copy(operator.at[rows, :], tile.at[t], sems.at[i, t])
            for i, (operator, tile) in enumerate(zip(operators, tiles))
        ]
        for copy in group:
            copy.start()
        copies.append(group)
    totals = [0.0] * pieces
    for t, group in enumerate(copies):
        source = own_ref if t < half else other_ref
        rows = source[:, (t % half) * depth:(t % half + 1) * depth]
        for i, copy in enumerate(group):
            copy.wait()
            totals[i] += jnp.dot(rows, tiles[i][t], preferred_element_type=jnp.float32)
    start = 0
    for total in totals:
        stop = start + total.shape[1]
        if add_ref is not None:
            total = total + add_ref[:, start:stop]
        out_ref[:, start:stop] = total.astype(out_ref.dtype)
        start = stop


def applied(own, other, pieces, addend=None):
    width = lax.axis_size("trace")
    rows = own.shape[0]
    deep = pieces[0].shape[0]
    columns = sum(piece.shape[1] for piece in pieces)
    vmem = pl.BlockSpec(memory_space=pltpu.VMEM)
    hbm = pl.BlockSpec(memory_space=pltpu.HBM)
    addends = [] if addend is None else [addend]
    return pl.pallas_call(
        functools.partial(apply_kernel, width, len(pieces)),
        out_shape=jax.ShapeDtypeStruct((rows, columns), jnp.bfloat16),
        in_specs=[vmem, vmem] + [hbm] * len(pieces) + [vmem] * len(addends),
        out_specs=vmem,
        scratch_shapes=[pltpu.VMEM((width, deep // width, piece.shape[1]), piece.dtype) for piece in pieces]
        + [pltpu.SemaphoreType.DMA((len(pieces), width))],
        compiler_params=pltpu.CompilerParams(vmem_limit_bytes=16 * 1024 * 1024),
        cost_estimate=pl.CostEstimate(
            flops=2 * rows * columns * deep, bytes_accessed=2 * columns * deep, transcendentals=0
        ),
    )(own, other, *pieces, *addends)


def in_turn(rows, pieces, addends, last):
    results = []
    for (own, other), addend in zip(rows, addends):
        last = applied(after(own, last), other, pieces, addend)
        results.append(last)
    return results


def shards(transmission, reflection, response, sources, placement):
    own_sources = sources[0]
    tick_count, batch_count, trace_width = own_sources.shape
    total_rows = tick_count * batch_count
    slab_index = lax.axis_index("slab")
    z = lax.axis_index("trace")
    trace_count = lax.axis_size("trace")
    places = Places(lax.axis_size("slab"), trace_count)
    core = slab_index % 2
    column = slab_index // 2
    my_stage = jnp.where(core == 0, column, places.columns - 1 - column)
    hops = range(1, places.extra + 1)

    distance = jnp.abs(slab_index - placement).astype(jnp.float32)
    weighting = 1.0 / (1.0 + distance)
    weighted = (own_sources.astype(jnp.float32) * weighting[:, :, None]).astype(jnp.bfloat16)
    flat = weighted.reshape(total_rows, trace_width)

    step = total_rows // CHUNKS

    def split(values):
        return [values[i * step:(i + 1) * step] for i in range(CHUNKS)]

    near_halves, far_halves = [], []
    for rows in split(flat):
        from_ends = [move(rows, places.exchange_end(hop)) for hop in hops]
        near = jnp.concatenate([rows] + from_ends, 1)
        far = move(near, places.swap_all())
        near_halves.append(near)
        far_halves.append(far)
    driven_parts = []
    for rows, near, far in zip(split(flat), near_halves, far_halves):
        far_outward = [move(far, places.outward(hop)) for hop in hops]
        near_outward = [] if places.extra == 1 else [move(near, places.outward(hop)) for hop in hops]
        if places.extra == 1:
            near_outward = [jnp.concatenate([near[:, trace_width:], rows], 1)]
        for hop, one_far, one_near in zip(hops, far_outward, near_outward):
            here = (z == places.ends(hop)[0][0]) | (z == places.ends(hop)[1][0])
            near, far = jnp.where(here, one_near, near), jnp.where(here, one_far, far)
        driven_parts.append(applied(near, far, [response[0]]))
    driven_sent = jnp.concatenate(driven_parts, 0)

    transfer = transmission[0]
    reflect = reflection[0]
    second_own = move(transfer, places.across_cores())
    second_early = joined([move(transfer, places.inward_crossed(hop, True)) for hop in hops])

    first_driven = jnp.concatenate(
        [driven_sent] + [move(driven_sent, places.exchange_end(hop)) for hop in hops], 1
    )
    late_source = after(transfer, first_driven)
    second_late = joined([move(late_source, places.inward_crossed(hop, False)) for hop in hops])

    firsts, seconds = [], []

    def chosen(stages, part):
        result = stages[0][part]
        for stage in range(1, places.columns):
            result = jnp.where(my_stage == stage, stages[stage][part], result)
        return result

    first_parts = split(first_driven)
    second_parts = split(move(first_driven, places.across_cores()))
    traces = first_parts
    for stage in range(places.columns):
        early = places.first_sender(stage) == 0
        second_pieces = [second_own] + (second_late if early else second_early)
        if stage:
            first_pieces = [transfer] + (first_early if early else first_late)
            arrived = []
            for part in traces:
                crossed = move(part, places.hop(stage, True))
                arrived.append((move(part, places.hop(stage, False)), crossed))
            traces = in_turn(arrived, first_pieces, first_parts, traces[-1])
        firsts.append(traces)
        others = []
        for part in traces:
            others.append(move(part, places.swap(stage)))
        traces = in_turn(list(zip(traces, others)), second_pieces, second_parts, traces[-1])
        seconds.append(traces)
        if stage == 0:
            first_early = [move(after(piece, traces[-1]), places.across_cores()) for piece in second_early]
        if stage == min(1, places.columns - 1):
            first_late = [move(after(piece, traces[-1]), places.across_cores()) for piece in second_late]
            reflect_source = after(reflect, traces[-1])
            reflect_rest = joined([move(reflect_source, places.inward(hop)) for hop in hops])

    outs = []
    for part in range(CHUNKS):
        mine = chosen(firsts, part).astype(jnp.float32)
        opposite = move(chosen(seconds, part), places.across_cores()).astype(jnp.float32)
        contrast = jnp.where(core == 0, mine - opposite, opposite - mine).astype(jnp.bfloat16)
        other = move(contrast, places.swap_all())
        combined = applied(contrast, other, [reflect] + reflect_rest, mine + opposite)
        own = combined[:, :trace_width]
        for hop in hops:
            piece = move(combined[:, hop * trace_width:(hop + 1) * trace_width], places.exchange_end(hop))
            own = jnp.where((z == places.ends(hop)[0][0]) | (z == places.ends(hop)[1][0]), piece, own)
        outs.append(own)
    return jnp.concatenate(outs, 0).reshape(1, tick_count, batch_count, trace_width)


def solution(mesh):
    placed = (
        P("slab", None, "trace"),
        P("slab", None, "trace"),
        P("slab", None, "trace"),
        P("slab", None, None, "trace"),
        P(),
    )

    return jax.shard_map(
        shards,
        mesh=mesh,
        in_specs=placed,
        out_specs=P("slab", None, None, "trace"),
        check_vma=False,
    )
```

```python
import functools

import jax
import jax.numpy as jnp
from jax import lax
from jax.experimental import pallas as pl
from jax.experimental.pallas import tpu as pltpu
from jax.sharding import PartitionSpec as P


AXES = ("slab", "trace")
CHUNKS = 2


class Places:
    def __init__(self, slab_count, trace_count):
        self.columns = slab_count // 2
        self.width = trace_count
        self.holders = (trace_count // 2 - 1, trace_count // 2)
        self.extra = trace_count // 2 - 1

    def at(self, column, core, z):
        return (2 * column + core) * self.width + z

    def everyone(self):
        return [(c, k, z) for c in range(self.columns) for k in (0, 1) for z in range(self.width)]

    def working(self, stage):
        return ((stage, 0), (self.columns - 1 - stage, 1))

    def partner_map(self):
        return {self.at(c, k, z): self.at(c, 1 - k, z) for c, k, z in self.everyone()}

    def across_cores(self):
        return list(self.partner_map().items())

    def swap(self, stage):
        moves = self.partner_map()
        (ca, ka), (cb, kb) = self.working(stage)
        low, high = self.holders
        for z, other in ((low, high), (high, low)):
            for c, k in ((ca, ka), (cb, kb)):
                moves[self.at(c, k, z)] = self.at(c, k, other)
            if ca != cb:
                moves[self.at(ca, 1 - ka, z)] = self.at(cb, 1 - kb, z)
                moves[self.at(cb, 1 - kb, z)] = self.at(ca, 1 - ka, z)
        return list(moves.items())

    def swap_all(self):
        moves = self.partner_map()
        low, high = self.holders
        for c in range(self.columns):
            for k in (0, 1):
                moves[self.at(c, k, low)] = self.at(c, k, high)
                moves[self.at(c, k, high)] = self.at(c, k, low)
        return list(moves.items())

    def hop(self, stage, crossed):
        moves = self.partner_map()
        low, high = self.holders
        for z, other in ((low, high), (high, low)):
            for (before, k), (after, _) in zip(self.working(stage - 1), self.working(stage)):
                moves[self.at(before, k, z)] = self.at(after, k, other if crossed else z)
                if 2 * stage != self.columns:
                    moves[self.at(after, 1 - k, z)] = self.at(before, 1 - k, z)
        return list(moves.items())

    def ends(self, hop):
        low, high = self.holders
        return ((low - hop, low), (high + hop, high))

    def exchange_end(self, hop):
        moves = []
        for c in range(self.columns):
            for k in (0, 1):
                for end, holder in self.ends(hop):
                    moves += [(self.at(c, k, end), self.at(c, k, holder)), (self.at(c, k, holder), self.at(c, k, end))]
        return moves

    def inward(self, hop):
        return [
            (self.at(c, k, end), self.at(c, k, holder))
            for c in range(self.columns) for k in (0, 1) for end, holder in self.ends(hop)
        ]

    def outward(self, hop):
        return [(holder, end) for end, holder in self.inward(hop)]

    def first_sender(self, column):
        if column < self.columns // 2:
            return 1 if column == 0 else 0
        return 1 - self.first_sender(self.columns - 1 - column)

    def inward_crossed(self, hop, early):
        moves = []
        for c in range(self.columns):
            k = self.first_sender(c) if early else 1 - self.first_sender(c)
            for end, holder in self.ends(hop):
                moves.append((self.at(c, k, end), self.at(c, 1 - k, holder)))
        return moves


def move(values, pairs):
    return lax.ppermute(values, AXES, pairs)


def after(values, earlier):
    return lax.optimization_barrier((values, earlier))[0]


def joined(pieces):
    return pieces if len(pieces) < 2 else [jnp.concatenate(pieces, 1)]


def apply_kernel(width, pieces, extras, turn, own_ref, other_ref, *refs):
    operators, rest = refs[:pieces], list(refs[pieces:])
    named = {name: rest.pop(0) for name in extras}
    out_ref = rest.pop(0)
    kept_ref = rest.pop(0) if "kept" in extras else None
    work = functools.partial(
        multiply, width, own_ref, other_ref, operators, named.get("addend"), out_ref, kept_ref, rest[:-1], rest[-1]
    )
    if turn is None:
        work()
        return
    z = lax.axis_index("trace")
    ours = (z == width // 2 - 1) | (z == width // 2)
    stage, columns = turn
    if stage is not None:
        slab = lax.axis_index("slab")
        column = lax.div(slab, 2)
        ours &= jnp.where(lax.rem(slab, 2) == 0, column, columns - 1 - column) == stage
    pl.when(ours)(work)
    if kept_ref is not None:
        @pl.when(jnp.logical_not(ours))
        def _():
            kept_ref[...] = named["kept"][...]


def multiply(width, own_ref, other_ref, operators, add_ref, out_ref, kept_ref, tiles, sems):
    pieces = len(operators)
    depth = operators[0].shape[0] // width
    half = width // 2
    lower = lax.axis_index("trace") < half
    down = [half - 1 - i for i in range(half)]
    up = [half + i for i in range(half)]
    blocks = [jnp.where(lower, x, y) for x, y in zip(down + up, up + down)]
    copies = []
    for t, block in enumerate(blocks):
        rows = pl.ds(pl.multiple_of(block * depth, depth), depth)
        group = [
            pltpu.make_async_copy(operator.at[rows, :], tile.at[t], sems.at[i, t])
            for i, (operator, tile) in enumerate(zip(operators, tiles))
        ]
        for copy in group:
            copy.start()
        copies.append(group)
    totals = [0.0] * pieces
    for t, group in enumerate(copies):
        source = own_ref if t < half else other_ref
        rows = source[:, (t % half) * depth:(t % half + 1) * depth]
        for i, copy in enumerate(group):
            copy.wait()
            totals[i] += jnp.dot(rows, tiles[i][t], preferred_element_type=jnp.float32)
    start = 0
    for total in totals:
        stop = start + total.shape[1]
        if add_ref is not None:
            total = total + add_ref[:, start:stop]
        result = total.astype(out_ref.dtype)
        out_ref[:, start:stop] = result
        if kept_ref is not None:
            kept_ref[:, start:stop] = result
        start = stop


def applied(own, other, pieces, addend=None, kept=None, turn=None):
    width = lax.axis_size("trace")
    rows = own.shape[0]
    deep = pieces[0].shape[0]
    columns = sum(piece.shape[1] for piece in pieces)
    vmem = pl.BlockSpec(memory_space=pltpu.VMEM)
    hbm = pl.BlockSpec(memory_space=pltpu.HBM)
    extras = {name: value for name, value in (("addend", addend), ("kept", kept)) if value is not None}
    outs = 1 if kept is None else 2
    return pl.pallas_call(
        functools.partial(apply_kernel, width, len(pieces), tuple(extras), turn),
        out_shape=[jax.ShapeDtypeStruct((rows, columns), jnp.bfloat16)] * outs,
        in_specs=[vmem, vmem] + [hbm] * len(pieces) + [vmem] * len(extras),
        out_specs=[vmem] * outs,
        scratch_shapes=[pltpu.VMEM((width, deep // width, piece.shape[1]), piece.dtype) for piece in pieces]
        + [pltpu.SemaphoreType.DMA((len(pieces), width))],
        compiler_params=pltpu.CompilerParams(vmem_limit_bytes=16 * 1024 * 1024),
        cost_estimate=pl.CostEstimate(
            flops=2 * rows * columns * deep, bytes_accessed=2 * columns * deep, transcendentals=0
        ),
    )(own, other, *pieces, *extras.values())


def in_turn(rows, pieces, addends, last, kept, turn):
    fresh = []
    for i, ((own, other), addend) in enumerate(zip(rows, addends)):
        outs = applied(after(own, last), other, pieces, addend, kept[i] if kept else None, turn)
        last = outs[0]
        fresh.append(outs)
    return [outs[0] for outs in fresh], [outs[-1] for outs in fresh]


def shards(transmission, reflection, response, sources, placement):
    own_sources = sources[0]
    tick_count, batch_count, trace_width = own_sources.shape
    total_rows = tick_count * batch_count
    slab_index = lax.axis_index("slab")
    z = lax.axis_index("trace")
    trace_count = lax.axis_size("trace")
    places = Places(lax.axis_size("slab"), trace_count)
    core = slab_index % 2
    hops = range(1, places.extra + 1)

    distance = jnp.abs(slab_index - placement).astype(jnp.float32)
    weighting = 1.0 / (1.0 + distance)
    weighted = (own_sources.astype(jnp.float32) * weighting[:, :, None]).astype(jnp.bfloat16)
    flat = weighted.reshape(total_rows, trace_width)

    step = total_rows // CHUNKS

    def split(values):
        return [values[i * step:(i + 1) * step] for i in range(CHUNKS)]

    near_halves, far_halves = [], []
    for rows in split(flat):
        from_ends = [move(rows, places.exchange_end(hop)) for hop in hops]
        near = jnp.concatenate([rows] + from_ends, 1)
        far = move(near, places.swap_all())
        near_halves.append(near)
        far_halves.append(far)
    driven_parts = []
    for rows, near, far in zip(split(flat), near_halves, far_halves):
        far_outward = [move(far, places.outward(hop)) for hop in hops]
        near_outward = [] if places.extra == 1 else [move(near, places.outward(hop)) for hop in hops]
        if places.extra == 1:
            near_outward = [jnp.concatenate([near[:, trace_width:], rows], 1)]
        for hop, one_far, one_near in zip(hops, far_outward, near_outward):
            here = (z == places.ends(hop)[0][0]) | (z == places.ends(hop)[1][0])
            near, far = jnp.where(here, one_near, near), jnp.where(here, one_far, far)
        driven_parts += applied(near, far, [response[0]])
    driven_sent = jnp.concatenate(driven_parts, 0)

    transfer = transmission[0]
    reflect = reflection[0]
    second_own = move(transfer, places.across_cores())
    second_early = joined([move(transfer, places.inward_crossed(hop, True)) for hop in hops])

    first_driven = jnp.concatenate(
        [driven_sent] + [move(driven_sent, places.exchange_end(hop)) for hop in hops], 1
    )
    late_source = after(transfer, first_driven)
    second_late = joined([move(late_source, places.inward_crossed(hop, False)) for hop in hops])

    first_parts = split(first_driven)
    second_parts = split(move(first_driven, places.across_cores()))
    traces = first_parts
    firsts, seconds = first_parts, None
    for stage in range(places.columns):
        turn = (stage, places.columns)
        early = places.first_sender(stage) == 0
        second_pieces = [second_own] + (second_late if early else second_early)
        if stage:
            first_pieces = [transfer] + (first_early if early else first_late)
            arrived = []
            for part in traces:
                crossed = move(part, places.hop(stage, True))
                arrived.append((move(part, places.hop(stage, False)), crossed))
            traces, firsts = in_turn(arrived, first_pieces, first_parts, traces[-1], firsts, turn)
        others = []
        for part in traces:
            others.append(move(part, places.swap(stage)))
        traces, seconds = in_turn(list(zip(traces, others)), second_pieces, second_parts, traces[-1], seconds, turn)
        if stage == 0:
            first_early = [move(after(piece, traces[-1]), places.across_cores()) for piece in second_early]
        if stage == min(1, places.columns - 1):
            first_late = [move(after(piece, traces[-1]), places.across_cores()) for piece in second_late]
            reflect_source = after(reflect, traces[-1])
            reflect_rest = joined([move(reflect_source, places.inward(hop)) for hop in hops])

    outs = []
    for part in range(CHUNKS):
        mine = firsts[part].astype(jnp.float32)
        opposite = move(seconds[part], places.across_cores()).astype(jnp.float32)
        contrast = jnp.where(core == 0, mine - opposite, opposite - mine).astype(jnp.bfloat16)
        other = move(contrast, places.swap_all())
        combined, = applied(
            contrast, other, [reflect] + reflect_rest, mine + opposite, turn=(None, places.columns)
        )
        own = combined[:, :trace_width]
        for hop in hops:
            piece = move(combined[:, hop * trace_width:(hop + 1) * trace_width], places.exchange_end(hop))
            own = jnp.where((z == places.ends(hop)[0][0]) | (z == places.ends(hop)[1][0]), piece, own)
        outs.append(own)
    return jnp.concatenate(outs, 0).reshape(1, tick_count, batch_count, trace_width)


def solution(mesh):
    placed = (
        P("slab", None, "trace"),
        P("slab", None, "trace"),
        P("slab", None, "trace"),
        P("slab", None, None, "trace"),
        P(),
    )

    return jax.shard_map(
        shards,
        mesh=mesh,
        in_specs=placed,
        out_specs=P("slab", None, None, "trace"),
        check_vma=False,
    )
```

```python
import functools

import jax
import jax.numpy as jnp
from jax import lax
from jax.experimental import pallas as pl
from jax.experimental.pallas import tpu as pltpu
from jax.sharding import PartitionSpec as P


AXES = ("slab", "trace")
CHUNKS = 2


class Places:
    def __init__(self, slab_count, trace_count):
        self.columns = slab_count // 2
        self.width = trace_count
        self.holders = (trace_count // 2 - 1, trace_count // 2)
        self.extra = trace_count // 2 - 1

    def at(self, column, core, z):
        return (2 * column + core) * self.width + z

    def everyone(self):
        return [(c, k, z) for c in range(self.columns) for k in (0, 1) for z in range(self.width)]

    def working(self, stage):
        return ((stage, 0), (self.columns - 1 - stage, 1))

    def partner_map(self):
        return {self.at(c, k, z): self.at(c, 1 - k, z) for c, k, z in self.everyone()}

    def across_cores(self):
        return list(self.partner_map().items())

    def swap(self, stage):
        moves = self.partner_map()
        (ca, ka), (cb, kb) = self.working(stage)
        low, high = self.holders
        for z, other in ((low, high), (high, low)):
            for c, k in ((ca, ka), (cb, kb)):
                moves[self.at(c, k, z)] = self.at(c, k, other)
            if ca != cb:
                moves[self.at(ca, 1 - ka, z)] = self.at(cb, 1 - kb, z)
                moves[self.at(cb, 1 - kb, z)] = self.at(ca, 1 - ka, z)
        return list(moves.items())

    def swap_all(self):
        moves = self.partner_map()
        low, high = self.holders
        for c in range(self.columns):
            for k in (0, 1):
                moves[self.at(c, k, low)] = self.at(c, k, high)
                moves[self.at(c, k, high)] = self.at(c, k, low)
        return list(moves.items())

    def hop(self, stage, crossed):
        moves = self.partner_map()
        low, high = self.holders
        for z, other in ((low, high), (high, low)):
            for (before, k), (after, _) in zip(self.working(stage - 1), self.working(stage)):
                moves[self.at(before, k, z)] = self.at(after, k, other if crossed else z)
                if 2 * stage != self.columns:
                    moves[self.at(after, 1 - k, z)] = self.at(before, 1 - k, z)
        return list(moves.items())

    def ends(self, hop):
        low, high = self.holders
        return ((low - hop, low), (high + hop, high))

    def exchange_end(self, hop):
        moves = []
        for c in range(self.columns):
            for k in (0, 1):
                for end, holder in self.ends(hop):
                    moves += [(self.at(c, k, end), self.at(c, k, holder)), (self.at(c, k, holder), self.at(c, k, end))]
        return moves

    def inward(self, hop):
        return [
            (self.at(c, k, end), self.at(c, k, holder))
            for c in range(self.columns) for k in (0, 1) for end, holder in self.ends(hop)
        ]

    def crossed_partners(self, moves, zs):
        (ca, ka), (cb, kb) = self.working(0)
        for z in zs:
            moves[self.at(ca, 1 - ka, z)] = self.at(cb, 1 - kb, z)
            moves[self.at(cb, 1 - kb, z)] = self.at(ca, 1 - ka, z)
        return list(moves.items())

    def swap_settled(self):
        moves = dict(self.swap_all())
        (ca, ka), (cb, kb) = self.working(0)
        for z in self.holders:
            moves[self.at(ca, ka, z)] = self.at(cb, kb, z)
            moves[self.at(cb, kb, z)] = self.at(ca, ka, z)
        return list(moves.items())

    def exchange_end_last(self, hop):
        moves = self.partner_map()
        for end, holder in self.ends(hop):
            for c, k in self.working(0):
                moves[self.at(c, k, end)] = self.at(c, k, holder)
                moves[self.at(c, k, holder)] = self.at(c, k, end)
        return self.crossed_partners(moves, [z for pair in self.ends(hop) for z in pair])

    def outward(self, hop):
        return [(holder, end) for end, holder in self.inward(hop)]

    def first_sender(self, column):
        if column < self.columns // 2:
            return 1 if column == 0 else 0
        return 1 - self.first_sender(self.columns - 1 - column)

    def inward_crossed(self, hop, early):
        moves = []
        for c in range(self.columns):
            k = self.first_sender(c) if early else 1 - self.first_sender(c)
            for end, holder in self.ends(hop):
                moves.append((self.at(c, k, end), self.at(c, 1 - k, holder)))
        return moves


def move(values, pairs):
    return lax.ppermute(values, AXES, pairs)


def after(values, earlier):
    return lax.optimization_barrier((values, earlier))[0]


def joined(pieces):
    return pieces if len(pieces) < 2 else [jnp.concatenate(pieces, 1)]


def apply_kernel(width, pieces, extras, turn, own_ref, other_ref, *refs):
    operators, rest = refs[:pieces], list(refs[pieces:])
    named = {name: rest.pop(0) for name in extras}
    out_ref = rest.pop(0)
    kept_ref = rest.pop(0) if "kept" in extras else None
    work = functools.partial(
        multiply, width, own_ref, other_ref, operators, named.get("addend"), out_ref, kept_ref, rest[:-1], rest[-1]
    )
    if turn is None:
        work()
        return
    z = lax.axis_index("trace")
    ours = (z == width // 2 - 1) | (z == width // 2)
    stage, columns, there = turn
    slab = lax.axis_index("slab")
    column = lax.div(slab, 2)
    ours &= (jnp.where(lax.rem(slab, 2) == 0, column, columns - 1 - column) == stage) == there
    pl.when(ours)(work)
    if kept_ref is not None:
        @pl.when(jnp.logical_not(ours))
        def _():
            kept_ref[...] = named["kept"][...]


def multiply(width, own_ref, other_ref, operators, add_ref, out_ref, kept_ref, tiles, sems):
    pieces = len(operators)
    depth = operators[0].shape[0] // width
    half = width // 2
    lower = lax.axis_index("trace") < half
    down = [half - 1 - i for i in range(half)]
    up = [half + i for i in range(half)]
    blocks = [jnp.where(lower, x, y) for x, y in zip(down + up, up + down)]
    copies = []
    for t, block in enumerate(blocks):
        rows = pl.ds(pl.multiple_of(block * depth, depth), depth)
        group = [
            pltpu.make_async_copy(operator.at[rows, :], tile.at[t], sems.at[i, t])
            for i, (operator, tile) in enumerate(zip(operators, tiles))
        ]
        for copy in group:
            copy.start()
        copies.append(group)
    totals = [0.0] * pieces
    for t, group in enumerate(copies):
        source = own_ref if t < half else other_ref
        rows = source[:, (t % half) * depth:(t % half + 1) * depth]
        for i, copy in enumerate(group):
            copy.wait()
            totals[i] += jnp.dot(rows, tiles[i][t], preferred_element_type=jnp.float32)
    start = 0
    for total in totals:
        stop = start + total.shape[1]
        if add_ref is not None:
            total = total + add_ref[:, start:stop]
        result = total.astype(out_ref.dtype)
        out_ref[:, start:stop] = result
        if kept_ref is not None:
            kept_ref[:, start:stop] = result
        start = stop


def applied(own, other, pieces, addend=None, kept=None, turn=None):
    width = lax.axis_size("trace")
    rows = own.shape[0]
    deep = pieces[0].shape[0]
    columns = sum(piece.shape[1] for piece in pieces)
    vmem = pl.BlockSpec(memory_space=pltpu.VMEM)
    hbm = pl.BlockSpec(memory_space=pltpu.HBM)
    extras = {name: value for name, value in (("addend", addend), ("kept", kept)) if value is not None}
    outs = 1 if kept is None else 2
    return pl.pallas_call(
        functools.partial(apply_kernel, width, len(pieces), tuple(extras), turn),
        out_shape=[jax.ShapeDtypeStruct((rows, columns), jnp.bfloat16)] * outs,
        in_specs=[vmem, vmem] + [hbm] * len(pieces) + [vmem] * len(extras),
        out_specs=[vmem] * outs,
        scratch_shapes=[pltpu.VMEM((width, deep // width, piece.shape[1]), piece.dtype) for piece in pieces]
        + [pltpu.SemaphoreType.DMA((len(pieces), width))],
        compiler_params=pltpu.CompilerParams(vmem_limit_bytes=16 * 1024 * 1024),
        cost_estimate=pl.CostEstimate(
            flops=2 * rows * columns * deep, bytes_accessed=2 * columns * deep, transcendentals=0
        ),
    )(own, other, *pieces, *extras.values())


def in_turn(rows, pieces, addends, last, kept, turn):
    fresh = []
    for i, ((own, other), addend) in enumerate(zip(rows, addends)):
        outs = applied(after(own, last), other, pieces, addend, kept[i] if kept else None, turn)
        last = outs[0]
        fresh.append(outs)
    return [outs[0] for outs in fresh], [outs[-1] for outs in fresh]


def shards(transmission, reflection, response, sources, placement):
    own_sources = sources[0]
    tick_count, batch_count, trace_width = own_sources.shape
    total_rows = tick_count * batch_count
    slab_index = lax.axis_index("slab")
    z = lax.axis_index("trace")
    trace_count = lax.axis_size("trace")
    places = Places(lax.axis_size("slab"), trace_count)
    core = slab_index % 2
    hops = range(1, places.extra + 1)

    distance = jnp.abs(slab_index - placement).astype(jnp.float32)
    weighting = 1.0 / (1.0 + distance)
    weighted = (own_sources.astype(jnp.float32) * weighting[:, :, None]).astype(jnp.bfloat16)
    flat = weighted.reshape(total_rows, trace_width)

    step = total_rows // CHUNKS

    def split(values):
        return [values[i * step:(i + 1) * step] for i in range(CHUNKS)]

    near_halves, far_halves = [], []
    for rows in split(flat):
        from_ends = [move(rows, places.exchange_end(hop)) for hop in hops]
        near = jnp.concatenate([rows] + from_ends, 1)
        far = move(near, places.swap_all())
        near_halves.append(near)
        far_halves.append(far)
    driven_parts = []
    for rows, near, far in zip(split(flat), near_halves, far_halves):
        far_outward = [move(far, places.outward(hop)) for hop in hops]
        near_outward = [] if places.extra == 1 else [move(near, places.outward(hop)) for hop in hops]
        if places.extra == 1:
            near_outward = [jnp.concatenate([near[:, trace_width:], rows], 1)]
        for hop, one_far, one_near in zip(hops, far_outward, near_outward):
            here = (z == places.ends(hop)[0][0]) | (z == places.ends(hop)[1][0])
            near, far = jnp.where(here, one_near, near), jnp.where(here, one_far, far)
        driven_parts += applied(near, far, [response[0]])
    driven_sent = jnp.concatenate(driven_parts, 0)

    transfer = transmission[0]
    reflect = reflection[0]
    second_own = move(transfer, places.across_cores())
    second_early = joined([move(transfer, places.inward_crossed(hop, True)) for hop in hops])

    first_driven = jnp.concatenate(
        [driven_sent] + [move(driven_sent, places.exchange_end(hop)) for hop in hops], 1
    )
    late_source = after(transfer, first_driven)
    second_late = joined([move(late_source, places.inward_crossed(hop, False)) for hop in hops])

    first_parts = split(first_driven)
    second_parts = split(move(first_driven, places.across_cores()))
    traces = first_parts
    firsts, seconds = first_parts, None
    for stage in range(places.columns):
        turn = (stage, places.columns, True)
        early = places.first_sender(stage) == 0
        second_pieces = [second_own] + (second_late if early else second_early)
        final = stage == places.columns - 1
        if final:
            settled = seconds
        if stage:
            first_pieces = [transfer] + (first_early if early else first_late)
            arrived = []
            for part in traces:
                crossed = move(part, places.hop(stage, True))
                arrived.append((move(part, places.hop(stage, False)), crossed))
            traces, firsts = in_turn(arrived, first_pieces, first_parts, traces[-1], firsts, turn)
        if final:
            given = []
            for part in settled:
                given.append(move(after(part, traces[-1]), places.across_cores()))
        others = []
        for part in traces:
            others.append(move(part, places.swap(stage)))
        traces, seconds = in_turn(list(zip(traces, others)), second_pieces, second_parts, traces[-1], seconds, turn)
        if stage == 0:
            first_early = [move(after(piece, traces[-1]), places.across_cores()) for piece in second_early]
        if stage == min(1, places.columns - 1):
            first_late = [move(after(piece, traces[-1]), places.across_cores()) for piece in second_late]
            reflect_source = after(reflect, traces[-1])
            reflect_rest = joined([move(reflect_source, places.inward(hop)) for hop in hops])

    def contrasts(ours, theirs):
        pairs = [(mine.astype(jnp.float32), other.astype(jnp.float32)) for mine, other in zip(ours, theirs)]
        return [
            (jnp.where(core == 0, mine - other, other - mine).astype(jnp.bfloat16), mine + other)
            for mine, other in pairs
        ]

    def swapped(rows, pairs):
        result = []
        for contrast, _ in rows:
            result.append(move(contrast, pairs))
        return result

    def sent_out(combined, pairs_of):
        result = []
        for rows in combined:
            result.append([
                move(rows[:, hop * trace_width:(hop + 1) * trace_width], pairs_of(hop)) for hop in hops
            ])
        return result

    reflect_pieces = [reflect] + reflect_rest
    settled_rows = contrasts(firsts, given)
    settled_others = swapped(settled_rows, places.swap_settled())
    last_given = []
    for part in seconds:
        last_given.append(move(part, places.across_cores()))
    last_rows = contrasts([after(mine, other) for mine, other in zip(firsts, last_given)], last_given)
    last_others = swapped(last_rows, places.swap(0))
    combined = []
    for (contrast, total), other in zip(settled_rows, settled_others):
        combined += applied(
            after(contrast, traces[-1]), other, reflect_pieces, total, turn=(0, places.columns, False)
        )
    settled_out = sent_out(combined, places.exchange_end)
    complete = []
    for (contrast, total), other, kept in zip(last_rows, last_others, combined):
        complete.append(applied(contrast, other, reflect_pieces, total, kept, (0, places.columns, True))[-1])
    last_out = sent_out(complete, places.exchange_end_last)
    in_last = (slab_index == 0) | (slab_index == 2 * places.columns - 1)
    outs = []
    for rows, from_settled, from_last in zip(complete, settled_out, last_out):
        own = rows[:, :trace_width]
        for hop, one, other in zip(hops, from_settled, from_last):
            here = (z == places.ends(hop)[0][0]) | (z == places.ends(hop)[1][0])
            own = jnp.where(here, jnp.where(in_last, other, one), own)
        outs.append(own)
    return jnp.concatenate(outs, 0).reshape(1, tick_count, batch_count, trace_width)


def solution(mesh):
    placed = (
        P("slab", None, "trace"),
        P("slab", None, "trace"),
        P("slab", None, "trace"),
        P("slab", None, None, "trace"),
        P(),
    )

    return jax.shard_map(
        shards,
        mesh=mesh,
        in_specs=placed,
        out_specs=P("slab", None, None, "trace"),
        check_vma=False,
    )
```

```python
import functools

import jax
import jax.numpy as jnp
from jax import lax
from jax.experimental import pallas as pl
from jax.experimental.pallas import tpu as pltpu
from jax.sharding import PartitionSpec as P


AXES = ("slab", "trace")
CHUNKS = 2


class Places:
    def __init__(self, slab_count, trace_count):
        self.columns = slab_count // 2
        self.width = trace_count
        self.holders = (trace_count // 2 - 1, trace_count // 2)
        self.extra = trace_count // 2 - 1

    def at(self, column, core, z):
        return (2 * column + core) * self.width + z

    def everyone(self):
        return [(c, k, z) for c in range(self.columns) for k in (0, 1) for z in range(self.width)]

    def working(self, stage):
        return ((stage, 0), (self.columns - 1 - stage, 1))

    def partner_map(self):
        return {self.at(c, k, z): self.at(c, 1 - k, z) for c, k, z in self.everyone()}

    def across_cores(self):
        return list(self.partner_map().items())

    def swap(self, stage):
        moves = self.partner_map()
        (ca, ka), (cb, kb) = self.working(stage)
        low, high = self.holders
        for z, other in ((low, high), (high, low)):
            for c, k in ((ca, ka), (cb, kb)):
                moves[self.at(c, k, z)] = self.at(c, k, other)
            if ca != cb:
                moves[self.at(ca, 1 - ka, z)] = self.at(cb, 1 - kb, z)
                moves[self.at(cb, 1 - kb, z)] = self.at(ca, 1 - ka, z)
        return list(moves.items())

    def swap_all(self):
        moves = self.partner_map()
        low, high = self.holders
        for c in range(self.columns):
            for k in (0, 1):
                moves[self.at(c, k, low)] = self.at(c, k, high)
                moves[self.at(c, k, high)] = self.at(c, k, low)
        return list(moves.items())

    def hop(self, stage, crossed):
        moves = self.partner_map()
        low, high = self.holders
        for z, other in ((low, high), (high, low)):
            for (before, k), (after, _) in zip(self.working(stage - 1), self.working(stage)):
                moves[self.at(before, k, z)] = self.at(after, k, other if crossed else z)
                if 2 * stage != self.columns:
                    moves[self.at(after, 1 - k, z)] = self.at(before, 1 - k, z)
        return list(moves.items())

    def ends(self, hop):
        low, high = self.holders
        return ((low - hop, low), (high + hop, high))

    def exchange_end(self, hop):
        moves = []
        for c in range(self.columns):
            for k in (0, 1):
                for end, holder in self.ends(hop):
                    moves += [(self.at(c, k, end), self.at(c, k, holder)), (self.at(c, k, holder), self.at(c, k, end))]
        return moves

    def inward(self, hop):
        return [
            (self.at(c, k, end), self.at(c, k, holder))
            for c in range(self.columns) for k in (0, 1) for end, holder in self.ends(hop)
        ]

    def crossed_partners(self, moves, zs):
        (ca, ka), (cb, kb) = self.working(0)
        for z in zs:
            moves[self.at(ca, 1 - ka, z)] = self.at(cb, 1 - kb, z)
            moves[self.at(cb, 1 - kb, z)] = self.at(ca, 1 - ka, z)
        return list(moves.items())

    def swap_settled(self):
        moves = dict(self.swap_all())
        (ca, ka), (cb, kb) = self.working(0)
        for z in self.holders:
            moves[self.at(ca, ka, z)] = self.at(cb, kb, z)
            moves[self.at(cb, kb, z)] = self.at(ca, ka, z)
        return list(moves.items())

    def exchange_end_last(self, hop):
        moves = self.partner_map()
        for end, holder in self.ends(hop):
            for c, k in self.working(0):
                moves[self.at(c, k, end)] = self.at(c, k, holder)
                moves[self.at(c, k, holder)] = self.at(c, k, end)
        return self.crossed_partners(moves, [z for pair in self.ends(hop) for z in pair])

    def outward(self, hop):
        return [(holder, end) for end, holder in self.inward(hop)]

    def first_sender(self, column):
        if column < self.columns // 2:
            return 1 if column == 0 else 0
        return 1 - self.first_sender(self.columns - 1 - column)

    def inward_crossed(self, hop, early):
        moves = []
        for c in range(self.columns):
            k = self.first_sender(c) if early else 1 - self.first_sender(c)
            for end, holder in self.ends(hop):
                moves.append((self.at(c, k, end), self.at(c, 1 - k, holder)))
        return moves


def move(values, pairs):
    return lax.ppermute(values, AXES, pairs)


def after(values, earlier):
    return lax.optimization_barrier((values, earlier))[0]


def joined(pieces):
    return pieces if len(pieces) < 2 else [jnp.concatenate(pieces, 1)]


def apply_kernel(width, pieces, extras, turn, own_ref, other_ref, *refs):
    operators, rest = refs[:pieces], list(refs[pieces:])
    named = {name: rest.pop(0) for name in extras}
    out_ref = rest.pop(0)
    kept_ref = rest.pop(0) if "kept" in extras else None
    work = functools.partial(
        multiply, width, own_ref, other_ref, operators, named.get("addend"), out_ref, kept_ref
    )
    if turn is None:
        work()
        return
    z = lax.axis_index("trace")
    ours = (z == width // 2 - 1) | (z == width // 2)
    stage, columns, there = turn
    slab = lax.axis_index("slab")
    column = lax.div(slab, 2)
    ours &= (jnp.where(lax.rem(slab, 2) == 0, column, columns - 1 - column) == stage) == there
    pl.when(ours)(work)
    if kept_ref is not None:
        @pl.when(jnp.logical_not(ours))
        def _():
            kept_ref[...] = named["kept"][...]


def multiply(width, own_ref, other_ref, operators, add_ref, out_ref, kept_ref):
    pieces = len(operators)
    depth = operators[0].shape[0] // width
    half = width // 2
    lower = lax.axis_index("trace") < half
    down = [half - 1 - i for i in range(half)]
    up = [half + i for i in range(half)]
    blocks = [jnp.where(lower, x, y) for x, y in zip(down + up, up + down)]
    totals = [0.0] * pieces
    for t, block in enumerate(blocks):
        source = own_ref if t < half else other_ref
        rows = source[:, (t % half) * depth:(t % half + 1) * depth]
        deep = pl.ds(pl.multiple_of(block * depth, depth), depth)
        for i, operator in enumerate(operators):
            totals[i] += jnp.dot(rows, operator[deep, :], preferred_element_type=jnp.float32)
    start = 0
    for total in totals:
        stop = start + total.shape[1]
        if add_ref is not None:
            total = total + add_ref[:, start:stop]
        result = total.astype(out_ref.dtype)
        out_ref[:, start:stop] = result
        if kept_ref is not None:
            kept_ref[:, start:stop] = result
        start = stop


def applied(own, other, pieces, addend=None, kept=None, turn=None):
    width = lax.axis_size("trace")
    rows = own.shape[0]
    deep = pieces[0].shape[0]
    columns = sum(piece.shape[1] for piece in pieces)
    vmem = pl.BlockSpec(memory_space=pltpu.VMEM)
    extras = {name: value for name, value in (("addend", addend), ("kept", kept)) if value is not None}
    outs = 1 if kept is None else 2
    return pl.pallas_call(
        functools.partial(apply_kernel, width, len(pieces), tuple(extras), turn),
        out_shape=[jax.ShapeDtypeStruct((rows, columns), jnp.bfloat16)] * outs,
        in_specs=[vmem] * (2 + len(pieces) + len(extras)),
        out_specs=[vmem] * outs,
        compiler_params=pltpu.CompilerParams(vmem_limit_bytes=8 * 1024 * 1024),
        cost_estimate=pl.CostEstimate(
            flops=2 * rows * columns * deep, bytes_accessed=2 * columns * deep, transcendentals=0
        ),
    )(own, other, *pieces, *extras.values())


def in_turn(rows, pieces, addends, last, kept, turn):
    fresh = []
    for i, ((own, other), addend) in enumerate(zip(rows, addends)):
        outs = applied(after(own, last), other, pieces, addend, kept[i] if kept else None, turn)
        last = outs[0]
        fresh.append(outs)
    return [outs[0] for outs in fresh], [outs[-1] for outs in fresh]


def shards(transmission, reflection, response, sources, placement):
    own_sources = sources[0]
    tick_count, batch_count, trace_width = own_sources.shape
    total_rows = tick_count * batch_count
    slab_index = lax.axis_index("slab")
    z = lax.axis_index("trace")
    trace_count = lax.axis_size("trace")
    places = Places(lax.axis_size("slab"), trace_count)
    core = slab_index % 2
    hops = range(1, places.extra + 1)

    distance = jnp.abs(slab_index - placement).astype(jnp.float32)
    weighting = 1.0 / (1.0 + distance)
    weighted = (own_sources.astype(jnp.float32) * weighting[:, :, None]).astype(jnp.bfloat16)
    flat = weighted.reshape(total_rows, trace_width)

    step = total_rows // CHUNKS

    def split(values):
        return [values[i * step:(i + 1) * step] for i in range(CHUNKS)]

    near_halves, far_halves = [], []
    for rows in split(flat):
        from_ends = [move(rows, places.exchange_end(hop)) for hop in hops]
        near = jnp.concatenate([rows] + from_ends, 1)
        far = move(near, places.swap_all())
        near_halves.append(near)
        far_halves.append(far)
    driven_parts = []
    for rows, near, far in zip(split(flat), near_halves, far_halves):
        far_outward = [move(far, places.outward(hop)) for hop in hops]
        near_outward = [] if places.extra == 1 else [move(near, places.outward(hop)) for hop in hops]
        if places.extra == 1:
            near_outward = [jnp.concatenate([near[:, trace_width:], rows], 1)]
        for hop, one_far, one_near in zip(hops, far_outward, near_outward):
            here = (z == places.ends(hop)[0][0]) | (z == places.ends(hop)[1][0])
            near, far = jnp.where(here, one_near, near), jnp.where(here, one_far, far)
        driven_parts += applied(near, far, [response[0]])
    driven_sent = jnp.concatenate(driven_parts, 0)

    transfer = transmission[0]
    reflect = reflection[0]
    second_own = move(transfer, places.across_cores())
    second_early = joined([move(transfer, places.inward_crossed(hop, True)) for hop in hops])

    first_driven = jnp.concatenate(
        [driven_sent] + [move(driven_sent, places.exchange_end(hop)) for hop in hops], 1
    )
    late_source = after(transfer, first_driven)
    second_late = joined([move(late_source, places.inward_crossed(hop, False)) for hop in hops])

    first_parts = split(first_driven)
    second_parts = split(move(first_driven, places.across_cores()))
    traces = first_parts
    firsts, seconds = first_parts, None
    for stage in range(places.columns):
        turn = (stage, places.columns, True)
        early = places.first_sender(stage) == 0
        second_pieces = [second_own] + (second_late if early else second_early)
        final = stage == places.columns - 1
        if final:
            settled = seconds
        if stage:
            first_pieces = [transfer] + (first_early if early else first_late)
            arrived = []
            for part in traces:
                crossed = move(part, places.hop(stage, True))
                arrived.append((move(part, places.hop(stage, False)), crossed))
            traces, firsts = in_turn(arrived, first_pieces, first_parts, traces[-1], firsts, turn)
        if final:
            given = []
            for part in settled:
                given.append(move(part, places.across_cores()))
        others = []
        for part in traces:
            others.append(move(part, places.swap(stage)))
        traces, seconds = in_turn(list(zip(traces, others)), second_pieces, second_parts, traces[-1], seconds, turn)
        if stage == 0:
            first_early = [move(after(piece, traces[-1]), places.across_cores()) for piece in second_early]
        if stage == min(1, places.columns - 1):
            first_late = [move(after(piece, traces[-1]), places.across_cores()) for piece in second_late]
            reflect_source = after(reflect, traces[-1])
            reflect_rest = joined([move(reflect_source, places.inward(hop)) for hop in hops])

    def contrasts(ours, theirs):
        pairs = [(mine.astype(jnp.float32), other.astype(jnp.float32)) for mine, other in zip(ours, theirs)]
        return [
            (jnp.where(core == 0, mine - other, other - mine).astype(jnp.bfloat16), mine + other)
            for mine, other in pairs
        ]

    def swapped(rows, pairs):
        result = []
        for contrast, _ in rows:
            result.append(move(contrast, pairs))
        return result

    def sent_out(combined, pairs_of):
        result = []
        for rows in combined:
            result.append([
                move(rows[:, hop * trace_width:(hop + 1) * trace_width], pairs_of(hop)) for hop in hops
            ])
        return result

    reflect_pieces = [reflect] + reflect_rest
    settled_rows = contrasts(firsts, given)
    settled_others = swapped(settled_rows, places.swap_settled())
    last_given = []
    for part in seconds:
        last_given.append(move(after(part, traces[-1]), places.across_cores()))
    last_rows = contrasts([after(mine, other) for mine, other in zip(firsts, last_given)], last_given)
    last_others = swapped(last_rows, places.swap(0))
    combined = []
    for (contrast, total), other in zip(settled_rows, settled_others):
        combined += applied(
            after(contrast, traces[-1]), other, reflect_pieces, total, turn=(0, places.columns, False)
        )
    settled_out = sent_out(combined, places.exchange_end)
    complete = []
    for (contrast, total), other, kept in zip(last_rows, last_others, combined):
        complete.append(applied(contrast, other, reflect_pieces, total, kept, (0, places.columns, True))[-1])
    last_out = sent_out(complete, places.exchange_end_last)
    in_last = (slab_index == 0) | (slab_index == 2 * places.columns - 1)
    outs = []
    for rows, from_settled, from_last in zip(complete, settled_out, last_out):
        own = rows[:, :trace_width]
        for hop, one, other in zip(hops, from_settled, from_last):
            here = (z == places.ends(hop)[0][0]) | (z == places.ends(hop)[1][0])
            own = jnp.where(here, jnp.where(in_last, other, one), own)
        outs.append(own)
    return jnp.concatenate(outs, 0).reshape(1, tick_count, batch_count, trace_width)


def solution(mesh):
    placed = (
        P("slab", None, "trace"),
        P("slab", None, "trace"),
        P("slab", None, "trace"),
        P("slab", None, None, "trace"),
        P(),
    )

    return jax.shard_map(
        shards,
        mesh=mesh,
        in_specs=placed,
        out_specs=P("slab", None, None, "trace"),
        check_vma=False,
    )
```

```python
import functools

import jax
import jax.numpy as jnp
from jax import lax
from jax.experimental import pallas as pl
from jax.experimental.pallas import tpu as pltpu
from jax.sharding import PartitionSpec as P


AXES = ("slab", "trace")
CHUNKS = 2


class Places:
    def __init__(self, slab_count, trace_count):
        self.columns = slab_count // 2
        self.width = trace_count
        self.holders = (trace_count // 2 - 1, trace_count // 2)
        self.extra = trace_count // 2 - 1

    def at(self, column, core, z):
        return (2 * column + core) * self.width + z

    def everyone(self):
        return [(c, k, z) for c in range(self.columns) for k in (0, 1) for z in range(self.width)]

    def working(self, stage):
        return ((stage, 0), (self.columns - 1 - stage, 1))

    def partner_map(self):
        return {self.at(c, k, z): self.at(c, 1 - k, z) for c, k, z in self.everyone()}

    def across_cores(self):
        return list(self.partner_map().items())

    def swap(self, stage):
        moves = self.partner_map()
        (ca, ka), (cb, kb) = self.working(stage)
        low, high = self.holders
        for z, other in ((low, high), (high, low)):
            for c, k in ((ca, ka), (cb, kb)):
                moves[self.at(c, k, z)] = self.at(c, k, other)
            if ca != cb:
                moves[self.at(ca, 1 - ka, z)] = self.at(cb, 1 - kb, z)
                moves[self.at(cb, 1 - kb, z)] = self.at(ca, 1 - ka, z)
        return list(moves.items())

    def swap_all(self):
        moves = self.partner_map()
        low, high = self.holders
        for c in range(self.columns):
            for k in (0, 1):
                moves[self.at(c, k, low)] = self.at(c, k, high)
                moves[self.at(c, k, high)] = self.at(c, k, low)
        return list(moves.items())

    def hop(self, stage, crossed):
        moves = self.partner_map()
        low, high = self.holders
        for z, other in ((low, high), (high, low)):
            for (before, k), (after, _) in zip(self.working(stage - 1), self.working(stage)):
                moves[self.at(before, k, z)] = self.at(after, k, other if crossed else z)
                if 2 * stage != self.columns:
                    moves[self.at(after, 1 - k, z)] = self.at(before, 1 - k, z)
        return list(moves.items())

    def ends(self, hop):
        low, high = self.holders
        return ((low - hop, low), (high + hop, high))

    def exchange_end(self, hop):
        moves = []
        for c in range(self.columns):
            for k in (0, 1):
                for end, holder in self.ends(hop):
                    moves += [(self.at(c, k, end), self.at(c, k, holder)), (self.at(c, k, holder), self.at(c, k, end))]
        return moves

    def inward(self, hop):
        return [
            (self.at(c, k, end), self.at(c, k, holder))
            for c in range(self.columns) for k in (0, 1) for end, holder in self.ends(hop)
        ]

    def outward(self, hop):
        return [(holder, end) for end, holder in self.inward(hop)]

    def first_sender(self, column):
        if column < self.columns // 2:
            return 1 if column == 0 else 0
        return 1 - self.first_sender(self.columns - 1 - column)

    def inward_crossed(self, hop, early):
        moves = []
        for c in range(self.columns):
            k = self.first_sender(c) if early else 1 - self.first_sender(c)
            for end, holder in self.ends(hop):
                moves.append((self.at(c, k, end), self.at(c, 1 - k, holder)))
        return moves


def move(values, pairs):
    return lax.ppermute(values, AXES, pairs)


def after(values, earlier):
    return lax.optimization_barrier((values, earlier))[0]


def joined(pieces):
    return pieces if len(pieces) < 2 else [jnp.concatenate(pieces, 1)]


def apply_kernel(width, pieces, extras, turn, own_ref, other_ref, *refs):
    operators, rest = refs[:pieces], list(refs[pieces:])
    named = {name: rest.pop(0) for name in extras}
    out_ref = rest.pop(0)
    kept_ref = rest.pop(0) if "kept" in extras else None
    work = functools.partial(
        multiply, width, own_ref, other_ref, operators, named.get("addend"), out_ref, kept_ref, rest[:-1], rest[-1:]
    )
    if turn is None:
        work()
        return
    z = lax.axis_index("trace")
    ours = (z == width // 2 - 1) | (z == width // 2)
    stage, columns = turn
    if stage is not None:
        slab = lax.axis_index("slab")
        column = lax.div(slab, 2)
        ours &= jnp.where(lax.rem(slab, 2) == 0, column, columns - 1 - column) == stage
    pl.when(ours)(work)
    if kept_ref is not None:
        @pl.when(jnp.logical_not(ours))
        def _():
            kept_ref[...] = named["kept"][...]


def multiply(width, own_ref, other_ref, operators, add_ref, out_ref, kept_ref, tiles, sems):
    pieces = len(operators)
    depth = operators[0].shape[0] // width
    half = width // 2
    lower = lax.axis_index("trace") < half
    down = [half - 1 - i for i in range(half)]
    up = [half + i for i in range(half)]
    blocks = [jnp.where(lower, x, y) for x, y in zip(down + up, up + down)]
    if not tiles:
        totals = [0.0] * pieces
        for t, block in enumerate(blocks):
            source = own_ref if t < half else other_ref
            rows = source[:, (t % half) * depth:(t % half + 1) * depth]
            deep = pl.ds(pl.multiple_of(block * depth, depth), depth)
            for i, operator in enumerate(operators):
                totals[i] += jnp.dot(rows, operator[deep, :], preferred_element_type=jnp.float32)
        finish(totals, add_ref, out_ref, kept_ref)
        return
    copies = []
    for t, block in enumerate(blocks):
        rows = pl.ds(pl.multiple_of(block * depth, depth), depth)
        group = [
            pltpu.make_async_copy(operator.at[rows, :], tile.at[t], sems[0].at[i, t])
            for i, (operator, tile) in enumerate(zip(operators, tiles))
        ]
        for copy in group:
            copy.start()
        copies.append(group)
    totals = [0.0] * pieces
    for t, group in enumerate(copies):
        source = own_ref if t < half else other_ref
        rows = source[:, (t % half) * depth:(t % half + 1) * depth]
        for i, copy in enumerate(group):
            copy.wait()
            totals[i] += jnp.dot(rows, tiles[i][t], preferred_element_type=jnp.float32)
    finish(totals, add_ref, out_ref, kept_ref)


def finish(totals, add_ref, out_ref, kept_ref):
    start = 0
    for total in totals:
        stop = start + total.shape[1]
        if add_ref is not None:
            total = total + add_ref[:, start:stop]
        result = total.astype(out_ref.dtype)
        out_ref[:, start:stop] = result
        if kept_ref is not None:
            kept_ref[:, start:stop] = result
        start = stop


def applied(own, other, pieces, addend=None, kept=None, turn=None, resident=False):
    width = lax.axis_size("trace")
    rows = own.shape[0]
    deep = pieces[0].shape[0]
    columns = sum(piece.shape[1] for piece in pieces)
    vmem = pl.BlockSpec(memory_space=pltpu.VMEM)
    hbm = pl.BlockSpec(memory_space=pltpu.HBM)
    extras = {name: value for name, value in (("addend", addend), ("kept", kept)) if value is not None}
    outs = 1 if kept is None else 2
    scratch = [] if resident else (
        [pltpu.VMEM((width, deep // width, piece.shape[1]), piece.dtype) for piece in pieces]
        + [pltpu.SemaphoreType.DMA((len(pieces), width))]
    )
    return pl.pallas_call(
        functools.partial(apply_kernel, width, len(pieces), tuple(extras), turn),
        out_shape=[jax.ShapeDtypeStruct((rows, columns), jnp.bfloat16)] * outs,
        in_specs=[vmem, vmem] + [vmem if resident else hbm] * len(pieces) + [vmem] * len(extras),
        out_specs=[vmem] * outs,
        scratch_shapes=scratch,
        compiler_params=pltpu.CompilerParams(vmem_limit_bytes=8 * 1024 * 1024),
        cost_estimate=pl.CostEstimate(
            flops=2 * rows * columns * deep, bytes_accessed=2 * columns * deep, transcendentals=0
        ),
    )(own, other, *pieces, *extras.values())


def in_turn(rows, pieces, addends, last, kept, turn, resident):
    fresh = []
    for i, ((own, other), addend) in enumerate(zip(rows, addends)):
        outs = applied(after(own, last), other, pieces, addend, kept[i] if kept else None, turn, resident)
        last = outs[0]
        fresh.append(outs)
    return [outs[0] for outs in fresh], [outs[-1] for outs in fresh]


def shards(transmission, reflection, response, sources, placement):
    own_sources = sources[0]
    tick_count, batch_count, trace_width = own_sources.shape
    total_rows = tick_count * batch_count
    slab_index = lax.axis_index("slab")
    z = lax.axis_index("trace")
    trace_count = lax.axis_size("trace")
    places = Places(lax.axis_size("slab"), trace_count)
    core = slab_index % 2
    hops = range(1, places.extra + 1)

    distance = jnp.abs(slab_index - placement).astype(jnp.float32)
    weighting = 1.0 / (1.0 + distance)
    weighted = (own_sources.astype(jnp.float32) * weighting[:, :, None]).astype(jnp.bfloat16)
    flat = weighted.reshape(total_rows, trace_width)

    step = total_rows // CHUNKS

    def split(values):
        return [values[i * step:(i + 1) * step] for i in range(CHUNKS)]

    near_halves, far_halves = [], []
    for rows in split(flat):
        from_ends = [move(rows, places.exchange_end(hop)) for hop in hops]
        near = jnp.concatenate([rows] + from_ends, 1)
        far = move(near, places.swap_all())
        near_halves.append(near)
        far_halves.append(far)
    driven_parts = []
    for rows, near, far in zip(split(flat), near_halves, far_halves):
        far_outward = [move(far, places.outward(hop)) for hop in hops]
        near_outward = [] if places.extra == 1 else [move(near, places.outward(hop)) for hop in hops]
        if places.extra == 1:
            near_outward = [jnp.concatenate([near[:, trace_width:], rows], 1)]
        for hop, one_far, one_near in zip(hops, far_outward, near_outward):
            here = (z == places.ends(hop)[0][0]) | (z == places.ends(hop)[1][0])
            near, far = jnp.where(here, one_near, near), jnp.where(here, one_far, far)
        driven_parts += applied(near, far, [response[0]], resident=True)
    driven_sent = jnp.concatenate(driven_parts, 0)

    transfer = transmission[0]
    reflect = reflection[0]
    second_own = move(transfer, places.across_cores())
    second_early = joined([move(transfer, places.inward_crossed(hop, True)) for hop in hops])

    first_driven = jnp.concatenate(
        [driven_sent] + [move(driven_sent, places.exchange_end(hop)) for hop in hops], 1
    )
    late_source = after(transfer, first_driven)
    second_late = joined([move(late_source, places.inward_crossed(hop, False)) for hop in hops])

    first_parts = split(first_driven)
    second_parts = split(move(first_driven, places.across_cores()))
    traces = first_parts
    firsts, seconds = first_parts, None
    for stage in range(places.columns):
        turn = (stage, places.columns)
        early = places.first_sender(stage) == 0
        second_pieces = [second_own] + (second_late if early else second_early)
        if stage:
            first_pieces = [transfer] + (first_early if early else first_late)
            arrived = []
            for part in traces:
                crossed = move(part, places.hop(stage, True))
                arrived.append((move(part, places.hop(stage, False)), crossed))
            traces, firsts = in_turn(arrived, first_pieces, first_parts, traces[-1], firsts, turn, True)
        others = []
        for part in traces:
            others.append(move(part, places.swap(stage)))
        traces, seconds = in_turn(list(zip(traces, others)), second_pieces, second_parts, traces[-1], seconds, turn, early)
        if stage == 0:
            first_early = [move(after(piece, traces[-1]), places.across_cores()) for piece in second_early]
        if stage == min(1, places.columns - 1):
            first_late = [move(after(piece, traces[-1]), places.across_cores()) for piece in second_late]
            reflect_source = after(reflect, traces[-1])
            reflect_rest = joined([move(reflect_source, places.inward(hop)) for hop in hops])

    outs = []
    for part in range(CHUNKS):
        mine = firsts[part].astype(jnp.float32)
        opposite = move(seconds[part], places.across_cores()).astype(jnp.float32)
        contrast = jnp.where(core == 0, mine - opposite, opposite - mine).astype(jnp.bfloat16)
        other = move(contrast, places.swap_all())
        combined, = applied(
            contrast, other, [reflect] + reflect_rest, mine + opposite, turn=(None, places.columns)
        )
        own = combined[:, :trace_width]
        for hop in hops:
            piece = move(combined[:, hop * trace_width:(hop + 1) * trace_width], places.exchange_end(hop))
            own = jnp.where((z == places.ends(hop)[0][0]) | (z == places.ends(hop)[1][0]), piece, own)
        outs.append(own)
    return jnp.concatenate(outs, 0).reshape(1, tick_count, batch_count, trace_width)


def solution(mesh):
    placed = (
        P("slab", None, "trace"),
        P("slab", None, "trace"),
        P("slab", None, "trace"),
        P("slab", None, None, "trace"),
        P(),
    )

    return jax.shard_map(
        shards,
        mesh=mesh,
        in_specs=placed,
        out_specs=P("slab", None, None, "trace"),
        check_vma=False,
    )
```

```python
import functools

import jax
import jax.numpy as jnp
from jax import lax
from jax.experimental import pallas as pl
from jax.experimental.pallas import tpu as pltpu
from jax.sharding import PartitionSpec as P


AXES = ("slab", "trace")
CHUNKS = 2


class Places:
    def __init__(self, slab_count, trace_count):
        self.columns = slab_count // 2
        self.width = trace_count
        self.holders = (trace_count // 2 - 1, trace_count // 2)
        self.extra = trace_count // 2 - 1

    def at(self, column, core, z):
        return (2 * column + core) * self.width + z

    def everyone(self):
        return [(c, k, z) for c in range(self.columns) for k in (0, 1) for z in range(self.width)]

    def working(self, stage):
        return ((stage, 0), (self.columns - 1 - stage, 1))

    def partner_map(self):
        return {self.at(c, k, z): self.at(c, 1 - k, z) for c, k, z in self.everyone()}

    def across_cores(self):
        return list(self.partner_map().items())

    def swap(self, stage):
        moves = self.partner_map()
        (ca, ka), (cb, kb) = self.working(stage)
        low, high = self.holders
        for z, other in ((low, high), (high, low)):
            for c, k in ((ca, ka), (cb, kb)):
                moves[self.at(c, k, z)] = self.at(c, k, other)
            if ca != cb:
                moves[self.at(ca, 1 - ka, z)] = self.at(cb, 1 - kb, z)
                moves[self.at(cb, 1 - kb, z)] = self.at(ca, 1 - ka, z)
        return list(moves.items())

    def swap_all(self):
        moves = self.partner_map()
        low, high = self.holders
        for c in range(self.columns):
            for k in (0, 1):
                moves[self.at(c, k, low)] = self.at(c, k, high)
                moves[self.at(c, k, high)] = self.at(c, k, low)
        return list(moves.items())

    def hop(self, stage, crossed):
        moves = self.partner_map()
        low, high = self.holders
        for z, other in ((low, high), (high, low)):
            for (before, k), (after, _) in zip(self.working(stage - 1), self.working(stage)):
                moves[self.at(before, k, z)] = self.at(after, k, other if crossed else z)
                if 2 * stage != self.columns:
                    moves[self.at(after, 1 - k, z)] = self.at(before, 1 - k, z)
        return list(moves.items())

    def ends(self, hop):
        low, high = self.holders
        return ((low - hop, low), (high + hop, high))

    def exchange_end(self, hop):
        moves = []
        for c in range(self.columns):
            for k in (0, 1):
                for end, holder in self.ends(hop):
                    moves += [(self.at(c, k, end), self.at(c, k, holder)), (self.at(c, k, holder), self.at(c, k, end))]
        return moves

    def inward(self, hop):
        return [
            (self.at(c, k, end), self.at(c, k, holder))
            for c in range(self.columns) for k in (0, 1) for end, holder in self.ends(hop)
        ]

    def outward(self, hop):
        return [(holder, end) for end, holder in self.inward(hop)]

    def first_sender(self, column):
        if column < self.columns // 2:
            return 1 if column == 0 else 0
        return 1 - self.first_sender(self.columns - 1 - column)

    def inward_crossed(self, hop, early):
        moves = []
        for c in range(self.columns):
            k = self.first_sender(c) if early else 1 - self.first_sender(c)
            for end, holder in self.ends(hop):
                moves.append((self.at(c, k, end), self.at(c, 1 - k, holder)))
        return moves


def move(values, pairs):
    return lax.ppermute(values, AXES, pairs)


def after(values, earlier):
    return lax.optimization_barrier((values, earlier))[0]


def joined(pieces):
    return pieces if len(pieces) < 2 else [jnp.concatenate(pieces, 1)]


def apply_kernel(width, pieces, extras, turn, own_ref, other_ref, *refs):
    operators, rest = refs[:pieces], list(refs[pieces:])
    named = {name: rest.pop(0) for name in extras}
    out_ref = rest.pop(0)
    kept_ref = rest.pop(0) if "kept" in extras else None
    work = functools.partial(
        multiply, width, own_ref, other_ref, operators, named.get("addend"), out_ref, kept_ref, rest[:-1], rest[-1:]
    )
    if turn is None:
        work()
        return
    z = lax.axis_index("trace")
    ours = (z == width // 2 - 1) | (z == width // 2)
    stage, columns = turn
    if stage is not None:
        slab = lax.axis_index("slab")
        column = lax.div(slab, 2)
        ours &= jnp.where(lax.rem(slab, 2) == 0, column, columns - 1 - column) == stage
    pl.when(ours)(work)
    if kept_ref is not None:
        @pl.when(jnp.logical_not(ours))
        def _():
            kept_ref[...] = named["kept"][...]


def multiply(width, own_ref, other_ref, operators, add_ref, out_ref, kept_ref, tiles, sems):
    pieces = len(operators)
    depth = operators[0].shape[0] // width
    half = width // 2
    lower = lax.axis_index("trace") < half
    down = [half - 1 - i for i in range(half)]
    up = [half + i for i in range(half)]
    blocks = [jnp.where(lower, x, y) for x, y in zip(down + up, up + down)]
    if not tiles:
        totals = [0.0] * pieces
        for t, block in enumerate(blocks):
            source = own_ref if t < half else other_ref
            rows = source[:, (t % half) * depth:(t % half + 1) * depth]
            deep = pl.ds(pl.multiple_of(block * depth, depth), depth)
            for i, operator in enumerate(operators):
                totals[i] += jnp.dot(rows, operator[deep, :], preferred_element_type=jnp.float32)
        finish(totals, add_ref, out_ref, kept_ref)
        return
    copies = []
    for t, block in enumerate(blocks):
        rows = pl.ds(pl.multiple_of(block * depth, depth), depth)
        group = [
            pltpu.make_async_copy(operator.at[rows, :], tile.at[t], sems[0].at[i, t])
            for i, (operator, tile) in enumerate(zip(operators, tiles))
        ]
        for copy in group:
            copy.start()
        copies.append(group)
    totals = [0.0] * pieces
    for t, group in enumerate(copies):
        source = own_ref if t < half else other_ref
        rows = source[:, (t % half) * depth:(t % half + 1) * depth]
        for i, copy in enumerate(group):
            copy.wait()
            totals[i] += jnp.dot(rows, tiles[i][t], preferred_element_type=jnp.float32)
    finish(totals, add_ref, out_ref, kept_ref)


def finish(totals, add_ref, out_ref, kept_ref):
    start = 0
    for total in totals:
        stop = start + total.shape[1]
        if add_ref is not None:
            total = total + add_ref[:, start:stop]
        result = total.astype(out_ref.dtype)
        out_ref[:, start:stop] = result
        if kept_ref is not None:
            kept_ref[:, start:stop] = result
        start = stop


def applied(own, other, pieces, addend=None, kept=None, turn=None, resident=False):
    width = lax.axis_size("trace")
    rows = own.shape[0]
    deep = pieces[0].shape[0]
    columns = sum(piece.shape[1] for piece in pieces)
    vmem = pl.BlockSpec(memory_space=pltpu.VMEM)
    hbm = pl.BlockSpec(memory_space=pltpu.HBM)
    extras = {name: value for name, value in (("addend", addend), ("kept", kept)) if value is not None}
    outs = 1 if kept is None else 2
    scratch = [] if resident else (
        [pltpu.VMEM((width, deep // width, piece.shape[1]), piece.dtype) for piece in pieces]
        + [pltpu.SemaphoreType.DMA((len(pieces), width))]
    )
    return pl.pallas_call(
        functools.partial(apply_kernel, width, len(pieces), tuple(extras), turn),
        out_shape=[jax.ShapeDtypeStruct((rows, columns), jnp.bfloat16)] * outs,
        in_specs=[vmem, vmem] + [vmem if resident else hbm] * len(pieces) + [vmem] * len(extras),
        out_specs=[vmem] * outs,
        scratch_shapes=scratch,
        compiler_params=pltpu.CompilerParams(vmem_limit_bytes=8 * 1024 * 1024),
        cost_estimate=pl.CostEstimate(
            flops=2 * rows * columns * deep, bytes_accessed=2 * columns * deep, transcendentals=0
        ),
    )(own, other, *pieces, *extras.values())


def in_turn(rows, pieces, addends, last, kept, turn, resident):
    fresh = []
    for i, ((own, other), addend) in enumerate(zip(rows, addends)):
        outs = applied(after(own, last), other, pieces, addend, kept[i] if kept else None, turn, resident)
        last = outs[0]
        fresh.append(outs)
    return [outs[0] for outs in fresh], [outs[-1] for outs in fresh]


def shards(transmission, reflection, response, sources, placement):
    own_sources = sources[0]
    tick_count, batch_count, trace_width = own_sources.shape
    total_rows = tick_count * batch_count
    slab_index = lax.axis_index("slab")
    z = lax.axis_index("trace")
    trace_count = lax.axis_size("trace")
    places = Places(lax.axis_size("slab"), trace_count)
    core = slab_index % 2
    hops = range(1, places.extra + 1)

    distance = jnp.abs(slab_index - placement).astype(jnp.float32)
    weighting = 1.0 / (1.0 + distance)
    weighted = (own_sources.astype(jnp.float32) * weighting[:, :, None]).astype(jnp.bfloat16)
    flat = weighted.reshape(total_rows, trace_width)

    step = total_rows // CHUNKS

    def split(values):
        return [values[i * step:(i + 1) * step] for i in range(CHUNKS)]

    near_halves, far_halves = [], []
    for rows in split(flat):
        from_ends = [move(rows, places.exchange_end(hop)) for hop in hops]
        near = jnp.concatenate([rows] + from_ends, 1)
        far = move(near, places.swap_all())
        near_halves.append(near)
        far_halves.append(far)
    driven_parts = []
    for rows, near, far in zip(split(flat), near_halves, far_halves):
        far_outward = [move(far, places.outward(hop)) for hop in hops]
        near_outward = [] if places.extra == 1 else [move(near, places.outward(hop)) for hop in hops]
        if places.extra == 1:
            near_outward = [jnp.concatenate([near[:, trace_width:], rows], 1)]
        for hop, one_far, one_near in zip(hops, far_outward, near_outward):
            here = (z == places.ends(hop)[0][0]) | (z == places.ends(hop)[1][0])
            near, far = jnp.where(here, one_near, near), jnp.where(here, one_far, far)
        driven_parts += applied(near, far, [response[0]], resident=True)
    driven_sent = jnp.concatenate(driven_parts, 0)

    transfer = transmission[0]
    reflect = reflection[0]
    second_own = move(transfer, places.across_cores())
    second_early = joined([move(transfer, places.inward_crossed(hop, True)) for hop in hops])

    first_driven = jnp.concatenate(
        [driven_sent] + [move(driven_sent, places.exchange_end(hop)) for hop in hops], 1
    )
    late_source = after(transfer, first_driven)
    second_late = joined([move(late_source, places.inward_crossed(hop, False)) for hop in hops])

    first_parts = split(first_driven)
    second_parts = split(move(first_driven, places.across_cores()))
    traces = first_parts
    firsts, seconds = first_parts, None
    for stage in range(places.columns):
        turn = (stage, places.columns)
        early = places.first_sender(stage) == 0
        second_pieces = [second_own] + (second_late if early else second_early)
        if stage:
            first_pieces = [transfer] + (first_early if early else first_late)
            arrived = []
            for part in traces:
                crossed = move(part, places.hop(stage, True))
                arrived.append((move(part, places.hop(stage, False)), crossed))
            traces, firsts = in_turn(arrived, first_pieces, first_parts, traces[-1], firsts, turn, True)
        others = []
        for part in traces:
            others.append(move(part, places.swap(stage)))
        traces, seconds = in_turn(
            list(zip(traces, others)), second_pieces, second_parts, traces[-1], seconds, turn, early
        )
        if stage == 0:
            first_early = [move(after(piece, traces[-1]), places.across_cores()) for piece in second_early]
        if stage == min(1, places.columns - 1):
            first_late = [move(after(piece, traces[-1]), places.across_cores()) for piece in second_late]
            reflect_source = after(reflect, traces[-1])
            reflect_rest = joined([move(reflect_source, places.inward(hop)) for hop in hops])

    outs = []
    for part in range(CHUNKS):
        mine = firsts[part].astype(jnp.float32)
        opposite = move(seconds[part], places.across_cores())
        opposite = opposite.astype(jnp.float32)
        contrast = jnp.where(core == 0, mine - opposite, opposite - mine).astype(jnp.bfloat16)
        other = move(contrast, places.swap_all())
        combined, = applied(
            contrast, other, [reflect] + reflect_rest, mine + opposite, turn=(None, places.columns)
        )
        own = combined[:, :trace_width]
        for hop in hops:
            piece = move(combined[:, hop * trace_width:(hop + 1) * trace_width], places.exchange_end(hop))
            own = jnp.where((z == places.ends(hop)[0][0]) | (z == places.ends(hop)[1][0]), piece, own)
        outs.append(own)
    return jnp.concatenate(outs, 0).reshape(1, tick_count, batch_count, trace_width)


def solution(mesh):
    placed = (
        P("slab", None, "trace"),
        P("slab", None, "trace"),
        P("slab", None, "trace"),
        P("slab", None, None, "trace"),
        P(),
    )

    return jax.shard_map(
        shards,
        mesh=mesh,
        in_specs=placed,
        out_specs=P("slab", None, None, "trace"),
        check_vma=False,
    )
```
